256 devices in a mesh: row: 16 (over z, core), col: 16 (over x, y).
Axes of the slice: x: 4, y: 4, z: 8, core: 2. Of those that a mesh axis runs over, the one named last changes fastest.
Arguments:
- grad: bfloat16 [2, 6144, 24576], P(None, 'row', 'col'), may hold values from -45 to 45, as said below
- memory: float32 [2, 6144, 24576], P(None, 'row', 'col'), may hold values from -6 to 6
- p_prev: float32 [2, 6144, 32], P(None, ('row', 'col')), may hold values from -6 to 6
- q_prev: float32 [2, 24576, 32], P(None, ('col', 'row')), may hold values from -1 to 1
Outputs:
- p_new: float32 [2, 6144, 32], P(None, ('row', 'col'))
- q_new: float32 [2, 24576, 32], P(None, ('col', 'row'))
- error: float32 [2, 6144, 24576], P(None, 'row', 'col')
The draws below stay inside these ranges and needn't reach their ends.
Inputs may be any that keep to these rules, and one draw needn't show every extreme that they name: `grad`: real-valued gradient entries.
All inputs are finite; a program needn't handle non-finite values.
Results may differ from the reference program's by a relative error of at most 0.0003.
Values sent between devices are 32-bit elements; how exact they have to be, the bound alone decides.
A program may use at most 64 MiB of HBM per device.

```python
import jax
import jax.numpy as jnp
from jax import lax

D = 6144
FF = 24576
R = 32
LAYERS = 2


def draw_grad(key, part):
    key_base = jax.random.fold_in(key, 11)
    key_rows = jax.random.fold_in(key, 12)
    key_cols = jax.random.fold_in(key, 13)
    base = jnp.clip(jax.random.normal(key_base, (LAYERS, D, FF), jnp.float32), -5.0, 5.0)
    row_scale = jnp.exp(jax.random.uniform(key_rows, (LAYERS, D, 1), jnp.float32, -1.2, 1.1))
    col_scale = jnp.exp(jax.random.uniform(key_cols, (LAYERS, 1, FF), jnp.float32, -1.2, 1.1))
    return (base * row_scale * col_scale).astype(jnp.bfloat16)


def levels(own_key, extent, split, least, largest):
    level, own = 1.0, jax.random.fold_in(own_key, 6)
    for dim, parts in split:
        steps = jnp.exp(jax.random.uniform(jax.random.fold_in(own, dim), (parts,), jnp.float32, least / len(split), largest / len(split)))
        level = level * jnp.repeat(steps, extent[dim] // parts).reshape([-1 if axis == dim else 1 for axis in range(len(extent))])
    return level


def bell_draw(rng, extent, width, most, pieces=(), held_as=jnp.bfloat16):
    entries = width * jax.random.normal(rng, extent, jnp.float32)
    if pieces:
        entries = entries * levels(rng, extent, pieces, -0.22, 0.18)
    return jnp.clip(entries, -most, most).astype(held_as)


def setup_inputs(seed: int = 0) -> dict:
    key_of = jax.random.split(jax.random.key(seed), 5)
    grad = draw_grad(jax.random.fold_in(key_of[4], 71), 0)
    memory = bell_draw(key_of[1], (LAYERS, D, FF), 1.0, 6.0, ((1, 16), (2, 16)), jnp.float32)
    p_prev = bell_draw(key_of[2], (LAYERS, D, R), 1.0, 6.0, ((1, 256),), jnp.float32)
    q_prev = bell_draw(key_of[3], (LAYERS, FF, R), R ** -0.5, 1.0, ((1, 256),), jnp.float32)
    return {"grad": grad, "memory": memory, "p_prev": p_prev, "q_prev": q_prev}


def reference(grad, memory, p_prev, q_prev):
    lefts = []
    rights = []
    errors = []
    for layer in range(LAYERS):
        approx = jnp.dot(p_prev[layer], q_prev[layer].T, precision=lax.Precision.HIGHEST)
        merged = grad[layer].astype(jnp.float32) + memory[layer] - approx
        left = jnp.dot(merged, q_prev[layer], precision=lax.Precision.HIGHEST)
        gram = jnp.dot(left.T, left, precision=lax.Precision.HIGHEST)
        factor = jnp.linalg.cholesky(gram)
        p_hat = lax.linalg.triangular_solve(factor, left, left_side=False, lower=True, transpose_a=True)
        right = jnp.dot(merged.T, p_hat, precision=lax.Precision.HIGHEST)
        error = merged - jnp.dot(p_hat, right.T, precision=lax.Precision.HIGHEST)
        lefts.append(p_hat)
        rights.append(right)
        errors.append(error)
    return (jnp.stack(lefts), jnp.stack(rights), jnp.stack(errors))
```

```python
import jax
import jax.numpy as jnp
from jax import lax
from jax.experimental import pallas as pl
from jax.experimental.pallas import tpu as pltpu
from jax.sharding import PartitionSpec as P

F32, BF16 = jnp.float32, jnp.bfloat16
HIGHEST = lax.Precision.HIGHEST
NT = (((1,), (1,)), ((), ()))
NN = (((1,), (0,)), ((), ()))
MESH = pl.DeviceIdType.MESH


def dot(a, b, dims=NN, precision=None):
    return lax.dot_general(a, b, dims, precision=precision, preferred_element_type=F32)


def pieces(v):
    first = v.astype(BF16).astype(F32)
    rest = v - first
    second = rest.astype(BF16).astype(F32)
    return first, second, rest - second


def shut(s):
    n = s.shape[1]
    low = jnp.concatenate([s[24:32, i * 32 : i * 32 + 32] for i in range(n // 32)], axis=0)
    return jnp.concatenate([s[0:24], low], axis=1)


def opened(p):
    low = jnp.concatenate([p[8 * i : 8 * i + 8, 96:128] for i in range(3)], axis=1)
    return jnp.concatenate([p[:, 0:96], low], axis=0)


def wide_left(p):
    a, b, c = pieces(p)
    return jnp.concatenate([a, a, a, b, b, c], axis=1).astype(BF16)


def tall_right(q):
    a, b, c = (v.astype(BF16) for v in pieces(q))
    return jnp.concatenate([a, b, c, a, b, a], axis=0)


def factor_kernel(
    zs, xs, ys,
    grad, memory, p_prev, q_prev,
    merged_out, wide_out, right_out, p_new, q_new,
    q_in, p_in, gbuf, tile, hi, lo, qg, pg, p_rows, wide, tall, b1, b2, left, gd, gz, rb, rd, rs, rr,
    load_sem, out_sem, zq_send, zq_recv, dq_send, dq_recv, p_send, p_recv, b_send, b_recv,
    gd_send, gd_recv, gz_send, gz_recv, rd_send, rd_recv, rz_send, rz_recv,
):
    layers, rows, cols = tile.shape
    row, col = lax.axis_index("row"), lax.axis_index("col")
    z, core = row // 2, row % 2
    x, y = col // ys, col % ys
    partner = {"row": z * 2 + (1 - core)}

    def z_peer(d):
        return {"row": ((z + d) % zs) * 2 + core}

    def x_peer(d):
        return {"col": ((x + d) % xs) * ys + y}

    def y_peer(d):
        return {"col": x * ys + (y + d) % ys}

    def remote(src, dst, send, recv, device):
        return pltpu.make_async_remote_copy(
            src_ref=src, dst_ref=dst, send_sem=send, recv_sem=recv, device_id=device, device_id_type=MESH
        )

    sent = []

    def start(copy):
        copy.start()
        sent.append(copy)
        return copy

    load_q = pltpu.make_async_copy(q_prev, q_in, load_sem.at[0])
    load_p = pltpu.make_async_copy(p_prev, p_in, load_sem.at[1])
    load_q.start()
    load_p.start()
    loads = []
    for l in range(layers):
        pair = (
            pltpu.make_async_copy(memory.at[l], tile.at[l], load_sem.at[2 + 2 * l]),
            pltpu.make_async_copy(grad.at[l], gbuf.at[l], load_sem.at[3 + 2 * l]),
        )
        for c in pair:
            c.start()
        loads.append(pair)

    barrier = pltpu.get_barrier_semaphore()
    peers = [partner] + [z_peer(d) for d in range(1, zs)]
    peers += [x_peer(d) for d in range(1, xs)] + [y_peer(d) for d in range(1, ys)]
    for device in peers:
        pl.semaphore_signal(barrier, inc=1, device_id=device, device_id_type=MESH)

    load_q.wait()
    for l in range(layers):
        qg[0, l, row] = shut(q_in[l].T)
    load_p.wait()
    for l in range(layers):
        p = p_in[l]
        pg[x, y, l] = jnp.concatenate([p[0:8], p[8:16], p[16:24], jnp.zeros((8, 32), F32)], axis=1)
    pl.semaphore_wait(barrier, len(peers))

    far_first = sorted(range(1, zs), key=lambda d: -min(d, zs - d))
    near_first = far_first[::-1]

    def send_shards(phase, l):
        mine = qg.at[phase, l, row]
        for d in far_first:
            start(remote(mine, mine, zq_send.at[phase, l, d], zq_recv.at[phase, l, d], z_peer(d)))
        start(remote(mine, mine, dq_send.at[phase, l, 0], dq_recv.at[phase, l, 0], partner))

    def pass_on(phase, l):
        for d in near_first:
            source = ((z + zs - d) % zs) * 2 + core
            there = qg.at[phase, l, source]
            remote(there, there, zq_send.at[phase, l, d], zq_recv.at[phase, l, d], z_peer(d)).wait_recv()
            start(remote(there, there, dq_send.at[phase, l, d], dq_recv.at[phase, l, d], partner))

    def all_passed(phase, l):
        for d in range(zs):
            other = ((z + zs - d) % zs) * 2 + (1 - core)
            there = qg.at[phase, l, other]
            remote(there, there, dq_send.at[phase, l, d], dq_recv.at[phase, l, d], partner).wait_recv()

    send_shards(0, 0)
    for d in range(1, ys):
        mine = pg.at[x, y]
        start(remote(mine, mine, p_send.at[0, d], p_recv.at[0, d], y_peer(d)))
    send_shards(0, 1)

    for l in range(layers):
        for c in loads[l]:
            c.wait()

        @pl.loop(0, rows // 32)
        def _(i):
            at = pl.ds(pl.multiple_of(i * 32, 32), 32)
            tile[l, at, :] = gbuf[l, at, :].astype(F32) + tile[l, at, :]

    for d in range(1, ys):
        there = pg.at[x, (y + ys - d) % ys]
        remote(there, there, p_send.at[0, d], p_recv.at[0, d], y_peer(d)).wait_recv()
    for d in range(1, xs):
        mine = pg.at[x]
        start(remote(mine, mine, p_send.at[1, d], p_recv.at[1, d], x_peer(d)))

    def q_columns(phase, l):
        return jnp.concatenate([opened(qg[phase, l, r]) for r in range(2 * zs)], axis=1)

    def merge(l):
        tall[...] = tall_right(q_columns(0, l))
        p = wide_left(p_rows[l])
        wide[...] = p
        acc = jnp.zeros((rows, 96), F32)
        step = 256
        for j in range(cols // step):
            at = pl.ds(j * step, step)
            m = tile[l, :, at] - dot(wide[...], tall[:, at])
            tile[l, :, at] = m
            m1 = m.astype(BF16)
            m2 = (m - m1.astype(F32)).astype(BF16)
            hi[l, :, at] = m1
            lo[l, :, at] = m2
            acc = acc + dot(m1, tall[0:96, at], NT) + dot(m2, tall[0:96, at], NT)
        part = acc[:, 0:32] + acc[:, 32:64] + acc[:, 64:96]
        return part

    half = rows // 2
    block = half // 4

    def halves(v):
        for h in range(2):
            yield jnp.concatenate([v[h * half + b * block : h * half + (b + 1) * block] for b in range(4)], axis=1)

    def exchange(buf, stage, l, h, along_y):
        n, me, peer = (ys, y, y_peer) if along_y else (xs, x, x_peer)
        mine = buf.at[l, h, me]
        for d in range(1, n):
            start(remote(mine, mine, b_send.at[stage, l, h, d], b_recv.at[stage, l, h, d], peer(d)))

    def arrived(buf, stage, l, h, along_y):
        n, me, peer = (ys, y, y_peer) if along_y else (xs, x, x_peer)
        for d in range(1, n):
            there = buf.at[l, h, (me + n - d) % n]
            remote(there, there, b_send.at[stage, l, h, d], b_recv.at[stage, l, h, d], peer(d)).wait_recv()
        total = buf[l, h, 0]
        for i in range(1, n):
            total = total + buf[l, h, i]
        return total

    def first_stage(l):
        part = merge(l)
        for h, v in enumerate(halves(part)):
            me = y if h == 0 else x
            b1[l, h, me] = v
            exchange(b1, 0, l, h, h == 0)
        pltpu.make_async_copy(tile.at[l], merged_out.at[l], out_sem.at[l]).start()

    def second_stage(l):
        for h in range(2):
            total = arrived(b1, 0, l, h, h == 0)
            me = x if h == 0 else y
            b2[l, h, me] = total
            exchange(b2, 1, l, h, h == 1)

    pass_on(0, 0)
    for d in range(1, xs):
        there = pg.at[(x + xs - d) % xs]
        remote(there, there, p_send.at[1, d], p_recv.at[1, d], x_peer(d)).wait_recv()
    for l in range(layers):
        for c in range(xs * ys):
            v = pg[c // ys, c % ys, l]
            p_rows[l, 24 * c : 24 * c + 24, :] = jnp.concatenate([v[:, 32 * b : 32 * b + 32] for b in range(3)], axis=0)
    all_passed(0, 0)
    first_stage(0)
    pass_on(0, 1)
    all_passed(0, 1)
    first_stage(1)
    second_stage(0)
    second_stage(1)

    def right_part(l):
        for h in range(2):
            total = arrived(b2, 1, l, h, h == 1)
            for b in range(4):
                left[l, h * half + b * block : h * half + (b + 1) * block, :] = total[:, 32 * b : 32 * b + 32]
        v = left[l]
        turned = v.T
        g = dot(turned, v, precision=HIGHEST)
        gd[l, core] = jnp.concatenate([g[8 * i : 8 * i + 8] for i in range(4)], axis=1)
        mine = gd.at[l, core]
        start(remote(mine, mine, gd_send.at[l], gd_recv.at[l], partner))
        t1, t2, t3 = (t.astype(BF16) for t in pieces(turned))
        lhs = jnp.concatenate([t1, t2, t3], axis=0)
        full = dot(lhs, hi[l]) + dot(lhs, lo[l])
        r = full[0:32] + full[32:64] + full[64:96]
        for s in range(2 * zs):
            rb[l, s % 2, s // 2] = shut(r[:, 96 * s : 96 * s + 96])
        start(remote(rb.at[l, 1 - core], rd.at[l], rd_send.at[l], rd_recv.at[l], partner))

    def send_gram(l):
        there = gd.at[l, 1 - core]
        remote(there, there, gd_send.at[l], gd_recv.at[l], partner).wait_recv()
        gz[l, z] = gd[l, 0] + gd[l, 1]
        mine = gz.at[l, z]
        for d in far_first:
            start(remote(mine, mine, gz_send.at[l, d], gz_recv.at[l, d], z_peer(d)))

    def scatter(l):
        remote(rb.at[l, 1 - core], rd.at[l], rd_send.at[l], rd_recv.at[l], partner).wait_recv()
        rs[l] = rb[l, core] + rd[l]
        for d in far_first:
            to = (z + d) % zs
            start(remote(rs.at[l, to], rr.at[l, z], rz_send.at[l, d], rz_recv.at[l, d], z_peer(d)))
        rr[l, z] = rs[l, z]

    right_part(0)
    send_gram(0)
    scatter(0)
    right_part(1)
    send_gram(1)
    scatter(1)

    def whole_gram(l):
        for d in range(1, zs):
            there = gz.at[l, (z + zs - d) % zs]
            remote(there, there, gz_send.at[l, d], gz_recv.at[l, d], z_peer(d)).wait_recv()
        g = gz[l, 0]
        for i in range(1, zs):
            g = g + gz[l, i]
        return jnp.concatenate([g[:, 32 * i : 32 * i + 32] for i in range(4)], axis=0)

    rank = 32
    ri = lax.broadcasted_iota(jnp.int32, (rank, 2 * rank), 0)
    ci = lax.broadcasted_iota(jnp.int32, (rank, 2 * rank), 1)
    eye = jnp.where(ri[:, 0:rank] == ci[:, 0:rank], 1.0, 0.0).astype(F32)
    sides = [jnp.concatenate([whole_gram(l), eye], axis=1) for l in range(layers)]
    for j in range(rank - 1):
        for l in range(layers):
            a = sides[l]
            pivot = a[j : j + 1, :]
            column = a[:, j : j + 1]
            scale = jnp.where(ri[:, 0:1] > j, column / a[j : j + 1, j : j + 1], 0.0)
            sides[l] = a - scale * pivot
    inverses = []
    for a in sides:
        diagonal = jnp.sum(jnp.where(ri == ci, a, 0.0), axis=1, keepdims=True)
        inverses.append(a[:, rank : 2 * rank] * lax.rsqrt(diagonal))

    def finish(l):
        for d in range(1, zs):
            there = rr.at[l, (z + zs - d) % zs]
            remote(rs.at[l, 0], there, rz_send.at[l, d], rz_recv.at[l, d], z_peer(d)).wait_recv()
        total = rr[l, 0]
        for i in range(1, zs):
            total = total + rr[l, i]
        q = dot(inverses[l], opened(total), precision=HIGHEST)
        qg[1, l, row] = shut(q)
        send_shards(1, l)
        q_new[l] = q.T

    finish(0)
    finish(1)
    for l in range(layers):
        p = dot(left[l], inverses[l], NT, precision=HIGHEST)
        p_rows[l] = p
        wide_out[l] = wide_left(p)
        share = rows // (xs * ys)
        p_new[l] = p_rows[l, pl.ds(pl.multiple_of(col * share, 8), share), :]
    for l in range(layers):
        pass_on(1, l)
    for l in range(layers):
        all_passed(1, l)
        right_out[l] = q_columns(1, l)
        pltpu.make_async_copy(tile.at[l], merged_out.at[l], out_sem.at[l]).wait()
    for copy in sent:
        copy.wait_send()


def error_kernel(merged, wide, right, error, buf, tall, in_sem, out_sem):
    layers, rows, cols = buf.shape
    step = 128

    def at(ref, l, i):
        return ref.at[l, pl.ds(i * step, step), :]

    order = [(l, i) for l in range(layers) for i in range(rows // step)]
    ins = [pltpu.make_async_copy(at(merged, l, i), at(buf, l, i), in_sem.at[l, i]) for l, i in order]
    outs = [pltpu.make_async_copy(at(buf, l, i), at(error, l, i), out_sem.at[l, i]) for l, i in order]
    for c in ins:
        c.start()
    for n, (l, i) in enumerate(order):
        if i == 0:
            tall[...] = tall_right(right[l])
        ins[n].wait()
        rows_at = pl.ds(i * step, step)
        buf[l, rows_at, :] = buf[l, rows_at, :] - dot(wide[l, rows_at, :], tall[...])
        outs[n].start()
    for c in outs:
        c.wait()


def shards(xs, ys, zs, grad, memory, p_prev, q_prev):
    layers, rows, cols = grad.shape
    rank = p_prev.shape[2]
    share, wire = q_prev.shape[1], 24
    dma = pltpu.SemaphoreType.DMA
    anywhere = pl.BlockSpec(memory_space=pl.ANY)
    vmem = pl.BlockSpec(memory_space=pltpu.VMEM)
    block = rows // 8

    def body(*refs):
        factor_kernel(zs, xs, ys, *refs)

    merged, wide, right, p_new, q_new = pl.pallas_call(
        body,
        out_shape=(
            jax.ShapeDtypeStruct((layers, rows, cols), F32),
            jax.ShapeDtypeStruct((layers, rows, 6 * rank), BF16),
            jax.ShapeDtypeStruct((layers, rank, cols), F32),
            jax.ShapeDtypeStruct(p_prev.shape, F32),
            jax.ShapeDtypeStruct(q_prev.shape, F32),
        ),
        in_specs=[anywhere] * 4,
        out_specs=(anywhere, vmem, vmem, vmem, vmem),
        scratch_shapes=[
            pltpu.VMEM(q_prev.shape, F32),
            pltpu.VMEM(p_prev.shape, F32),
            pltpu.VMEM((layers, rows, cols), BF16),
            pltpu.VMEM((layers, rows, cols), F32),
            pltpu.VMEM((layers, rows, cols), BF16),
            pltpu.VMEM((layers, rows, cols), BF16),
            pltpu.VMEM((2, layers, 2 * zs, wire, 128), F32),
            pltpu.VMEM((xs, ys, layers, 8, 128), F32),
            pltpu.VMEM((layers, rows, rank), F32),
            pltpu.VMEM((rows, 6 * rank), BF16),
            pltpu.VMEM((6 * rank, cols), BF16),
            pltpu.VMEM((layers, 2, 4, block, 128), F32),
            pltpu.VMEM((layers, 2, 4, block, 128), F32),
            pltpu.VMEM((layers, rows, rank), F32),
            pltpu.VMEM((layers, 2, 8, 128), F32),
            pltpu.VMEM((layers, zs, 8, 128), F32),
            pltpu.VMEM((layers, 2, zs, wire, 128), F32),
            pltpu.VMEM((layers, zs, wire, 128), F32),
            pltpu.VMEM((layers, zs, wire, 128), F32),
            pltpu.VMEM((layers, zs, wire, 128), F32),
            dma((2 + 2 * layers,)),
            dma((layers,)),
            dma((2, layers, zs)),
            dma((2, layers, zs)),
            dma((2, layers, zs)),
            dma((2, layers, zs)),
            dma((2, 4)),
            dma((2, 4)),
            dma((2, layers, 2, 4)),
            dma((2, layers, 2, 4)),
            dma((layers,)),
            dma((layers,)),
            dma((layers, zs)),
            dma((layers, zs)),
            dma((layers,)),
            dma((layers,)),
            dma((layers, zs)),
            dma((layers, zs)),
        ],
        compiler_params=pltpu.CompilerParams(
            collective_id=0, has_side_effects=True, vmem_limit_bytes=48 * 1024 * 1024
        ),
        name="factors",
    )(grad, memory, p_prev, q_prev)
    error = pl.pallas_call(
        error_kernel,
        out_shape=jax.ShapeDtypeStruct((layers, rows, cols), F32),
        in_specs=[anywhere, vmem, vmem],
        out_specs=anywhere,
        scratch_shapes=[
            pltpu.VMEM((layers, rows, cols), F32),
            pltpu.VMEM((6 * rank, cols), BF16),
            dma((layers, rows // 128)),
            dma((layers, rows // 128)),
        ],
        compiler_params=pltpu.CompilerParams(vmem_limit_bytes=32 * 1024 * 1024),
        name="error",
    )(merged, wide, right)
    return p_new, q_new, error


def solution(mesh):
    placed = (
        P(None, "row", "col"),
        P(None, "row", "col"),
        P(None, ("row", "col"), None),
        P(None, ("col", "row"), None),
    )
    xs = ys = 4
    zs = mesh.shape["row"] // 2

    def body(grad, memory, p_prev, q_prev):
        return shards(xs, ys, zs, grad, memory, p_prev, q_prev)

    return jax.shard_map(
        body,
        mesh=mesh,
        in_specs=placed,
        out_specs=(
            P(None, ("row", "col"), None),
            P(None, ("col", "row"), None),
            P(None, "row", "col"),
        ),
        check_vma=False,
    )
```

```python
import jax
import jax.numpy as jnp
from jax import lax
from jax.experimental import pallas as pl
from jax.experimental.pallas import tpu as pltpu
from jax.sharding import PartitionSpec as P

F32, BF16 = jnp.float32, jnp.bfloat16
HIGHEST = lax.Precision.HIGHEST
NT = (((1,), (1,)), ((), ()))
NN = (((1,), (0,)), ((), ()))
MESH = pl.DeviceIdType.MESH


def dot(a, b, dims=NN, precision=None):
    return lax.dot_general(a, b, dims, precision=precision, preferred_element_type=F32)


def pieces(v):
    first = v.astype(BF16).astype(F32)
    rest = v - first
    second = rest.astype(BF16).astype(F32)
    return first, second, rest - second


def shut(s):
    n = s.shape[1]
    low = jnp.concatenate([s[24:32, i * 32 : i * 32 + 32] for i in range(n // 32)], axis=0)
    return jnp.concatenate([s[0:24], low], axis=1)


def opened(p):
    low = jnp.concatenate([p[8 * i : 8 * i + 8, 96:128] for i in range(3)], axis=1)
    return jnp.concatenate([p[:, 0:96], low], axis=0)


def wide_left(p):
    a, b, c = pieces(p)
    return jnp.concatenate([a, a, a, b, b, c], axis=1).astype(BF16)


def tall_right(q):
    a, b, c = (v.astype(BF16) for v in pieces(q))
    return jnp.concatenate([a, b, c, a, b, a], axis=0)


def factor_kernel(
    zs, xs, ys,
    grad, memory, p_prev, q_prev,
    tile, wide_out, right_out, p_new, q_new,
    q_in, p_in, gbuf, hi, lo, qg, pg, p_rows, wide, tall, b1, b2, left, gd, gz, rb, rd, rs, rr,
    load_sem, zq_send, zq_recv, dq_send, dq_recv, p_send, p_recv, b_send, b_recv,
    gd_send, gd_recv, gz_send, gz_recv, rd_send, rd_recv, rz_send, rz_recv,
):
    layers, rows, cols = tile.shape
    row, col = lax.axis_index("row"), lax.axis_index("col")
    z, core = row // 2, row % 2
    x, y = col // ys, col % ys
    partner = {"row": z * 2 + (1 - core)}

    def z_peer(d):
        return {"row": ((z + d) % zs) * 2 + core}

    def xy_peer(dx, dy):
        return {"col": lax.rem(x + dx, xs) * ys + lax.rem(y + dy, ys)}

    def x_peer(d):
        return {"col": ((x + d) % xs) * ys + y}

    def y_peer(d):
        return {"col": x * ys + (y + d) % ys}

    def remote(src, dst, send, recv, device):
        return pltpu.make_async_remote_copy(
            src_ref=src, dst_ref=dst, send_sem=send, recv_sem=recv, device_id=device, device_id_type=MESH
        )

    sent = []

    def start(copy):
        copy.start()
        sent.append(copy)
        return copy

    load_q = pltpu.make_async_copy(q_prev, q_in, load_sem.at[0])
    load_p = pltpu.make_async_copy(p_prev, p_in, load_sem.at[1])
    load_q.start()
    load_p.start()
    loads = []
    for l in range(layers):
        pair = (
            pltpu.make_async_copy(memory.at[l], tile.at[l], load_sem.at[2 + 2 * l]),
            pltpu.make_async_copy(grad.at[l], gbuf.at[l], load_sem.at[3 + 2 * l]),
        )
        for c in pair:
            c.start()
        loads.append(pair)

    barrier = pltpu.get_barrier_semaphore()
    peers = [partner] + [z_peer(d) for d in range(1, zs)]
    offsets = [(dx, dy) for dx in (2, 1, 3, 0) for dy in (2, 1, 3, 0) if dx or dy]
    peers += [xy_peer(dx, dy) for dx, dy in offsets]
    for device in peers:
        pl.semaphore_signal(barrier, inc=1, device_id=device, device_id_type=MESH)

    load_q.wait()
    for l in range(layers):
        qg[0, l, row] = shut(q_in[l])
    load_p.wait()
    for l in range(layers):
        p = p_in[l]
        pg[x, y, l] = jnp.concatenate([p[0:8], p[8:16], p[16:24], jnp.zeros((8, 32), F32)], axis=1)
    for l in range(layers):
        for c in loads[l]:
            c.wait()

        @pl.loop(0, rows // 32)
        def _(i):
            at = pl.ds(pl.multiple_of(i * 32, 32), 32)
            t = gbuf[l, at, :].astype(F32) + tile[l, at, :]
            tile[l, at, :] = t
            t1 = t.astype(BF16)
            hi[l, at, :] = t1
            lo[l, at, :] = (t - t1.astype(F32)).astype(BF16)

    pl.semaphore_wait(barrier, len(peers))

    far_first = sorted(range(1, zs), key=lambda d: -min(d, zs - d))
    near_first = far_first[::-1]

    def send_shards(phase, l):
        mine = qg.at[phase, l, row]
        for d in far_first:
            start(remote(mine, mine, zq_send.at[phase, l, d], zq_recv.at[phase, l, d], z_peer(d)))
        start(remote(mine, mine, dq_send.at[phase, l, 0], dq_recv.at[phase, l, 0], partner))

    def pass_on(phase, l):
        for d in near_first:
            source = ((z + zs - d) % zs) * 2 + core
            there = qg.at[phase, l, source]
            remote(there, there, zq_send.at[phase, l, d], zq_recv.at[phase, l, d], z_peer(d)).wait_recv()
            start(remote(there, there, dq_send.at[phase, l, d], dq_recv.at[phase, l, d], partner))

    def all_passed(phase, l):
        for d in range(zs):
            other = ((z + zs - d) % zs) * 2 + (1 - core)
            there = qg.at[phase, l, other]
            remote(there, there, dq_send.at[phase, l, d], dq_recv.at[phase, l, d], partner).wait_recv()

    send_shards(0, 0)
    for dx, dy in offsets:
        mine = pg.at[x, y]
        start(remote(mine, mine, p_send.at[dx, dy], p_recv.at[dx, dy], xy_peer(dx, dy)))
    send_shards(0, 1)

    def q_columns(phase, l):
        return jnp.concatenate([opened(qg[phase, l, r]) for r in range(2 * zs)], axis=1)

    step = 256

    def left_part(l):
        tall[l] = tall_right(q_columns(0, l))
        wide[l] = wide_left(p_rows[l])
        q3 = tall[l, 0:96, :]
        acc = dot(hi[l], q3, NT) + dot(lo[l], q3, NT)
        square = dot(q3, q3, NT)
        square = square[0:32] + square[32:64] + square[64:96]
        square = square[:, 0:32] + square[:, 32:64] + square[:, 64:96]
        part = acc[:, 0:32] + acc[:, 32:64] + acc[:, 64:96]
        return part - dot(wide[l], tall_right(square))

    def merge(l):
        for j in range(cols // step):
            at = pl.ds(j * step, step)
            m = tile[l, :, at] - dot(wide[l], tall[l, :, at])
            tile[l, :, at] = m
            m1 = m.astype(BF16)
            hi[l, :, at] = m1
            lo[l, :, at] = (m - m1.astype(F32)).astype(BF16)

    half = rows // 2
    block = half // 4

    def halves(v):
        for h in range(2):
            yield jnp.concatenate([v[h * half + b * block : h * half + (b + 1) * block] for b in range(4)], axis=1)

    def exchange(buf, stage, l, h, along_y):
        n, me, peer = (ys, y, y_peer) if along_y else (xs, x, x_peer)
        mine = buf.at[l, h, me]
        for d in range(1, n):
            start(remote(mine, mine, b_send.at[stage, l, h, d], b_recv.at[stage, l, h, d], peer(d)))

    def arrived(buf, stage, l, h, along_y):
        n, me, peer = (ys, y, y_peer) if along_y else (xs, x, x_peer)
        for d in range(1, n):
            there = buf.at[l, h, (me + n - d) % n]
            remote(there, there, b_send.at[stage, l, h, d], b_recv.at[stage, l, h, d], peer(d)).wait_recv()
        total = buf[l, h, 0]
        for i in range(1, n):
            total = total + buf[l, h, i]
        return total

    def first_stage(l):
        part = left_part(l)
        for h, v in enumerate(halves(part)):
            me = y if h == 0 else x
            b1[l, h, me] = v
            exchange(b1, 0, l, h, h == 0)

    def second_stage(l):
        for h in range(2):
            total = arrived(b1, 0, l, h, h == 0)
            me = x if h == 0 else y
            b2[l, h, me] = total
            exchange(b2, 1, l, h, h == 1)

    pass_on(0, 0)
    for dx, dy in offsets[::-1]:
        there = pg.at[lax.rem(x + xs - dx, xs), lax.rem(y + ys - dy, ys)]
        remote(there, there, p_send.at[dx, dy], p_recv.at[dx, dy], xy_peer(dx, dy)).wait_recv()
    for l in range(layers):
        for c in range(xs * ys):
            v = pg[c // ys, c % ys, l]
            p_rows[l, 24 * c : 24 * c + 24, :] = jnp.concatenate([v[:, 32 * b : 32 * b + 32] for b in range(3)], axis=0)
    pass_on(0, 1)
    all_passed(0, 0)
    first_stage(0)
    all_passed(0, 1)
    first_stage(1)
    merge(0)
    merge(1)
    second_stage(0)
    second_stage(1)

    def right_part(l):
        for h in range(2):
            total = arrived(b2, 1, l, h, h == 1)
            for b in range(4):
                left[l, h * half + b * block : h * half + (b + 1) * block, :] = total[:, 32 * b : 32 * b + 32]
        v = left[l]
        turned = v.T
        g = dot(turned, v, precision=HIGHEST)
        gd[l, core] = jnp.concatenate([g[8 * i : 8 * i + 8] for i in range(4)], axis=1)
        mine = gd.at[l, core]
        start(remote(mine, mine, gd_send.at[l], gd_recv.at[l], partner))
        t1, t2, t3 = (t.astype(BF16) for t in pieces(turned))
        lhs = jnp.concatenate([t1, t2, t3], axis=0)
        full = dot(lhs, hi[l]) + dot(lhs, lo[l])
        r = full[0:32] + full[32:64] + full[64:96]
        for s in range(2 * zs):
            rb[l, s % 2, s // 2] = shut(r[:, 96 * s : 96 * s + 96])
        start(remote(rb.at[l, 1 - core], rd.at[l], rd_send.at[l], rd_recv.at[l], partner))

    def send_gram(l):
        there = gd.at[l, 1 - core]
        remote(there, there, gd_send.at[l], gd_recv.at[l], partner).wait_recv()
        gz[l, z] = gd[l, 0] + gd[l, 1]
        mine = gz.at[l, z]
        for d in far_first:
            start(remote(mine, mine, gz_send.at[l, d], gz_recv.at[l, d], z_peer(d)))

    def scatter(l):
        remote(rb.at[l, 1 - core], rd.at[l], rd_send.at[l], rd_recv.at[l], partner).wait_recv()
        rs[l] = rb[l, core] + rd[l]
        for d in far_first:
            to = (z + d) % zs
            start(remote(rs.at[l, to], rr.at[l, z], rz_send.at[l, d], rz_recv.at[l, d], z_peer(d)))
        rr[l, z] = rs[l, z]

    right_part(0)
    send_gram(0)
    right_part(1)
    scatter(0)
    send_gram(1)
    scatter(1)

    def gather(l):
        for d in near_first:
            there = rr.at[l, (z + zs - d) % zs]
            remote(rs.at[l, 0], there, rz_send.at[l, d], rz_recv.at[l, d], z_peer(d)).wait_recv()
        total = rr[l, 0]
        for i in range(1, zs):
            total = total + rr[l, i]
        qg[1, l, row] = total
        send_shards(1, l)

    gather(0)
    gather(1)

    def whole_gram(l):
        for d in range(1, zs):
            there = gz.at[l, (z + zs - d) % zs]
            remote(there, there, gz_send.at[l, d], gz_recv.at[l, d], z_peer(d)).wait_recv()
        g = gz[l, 0]
        for i in range(1, zs):
            g = g + gz[l, i]
        return jnp.concatenate([g[:, 32 * i : 32 * i + 32] for i in range(4)], axis=0)

    rank = 32
    ri = lax.broadcasted_iota(jnp.int32, (rank, 2 * rank), 0)
    ci = lax.broadcasted_iota(jnp.int32, (rank, 2 * rank), 1)
    eye = jnp.where(ri[:, 0:rank] == ci[:, 0:rank], 1.0, 0.0).astype(F32)
    sides = [jnp.concatenate([whole_gram(l), eye], axis=1) for l in range(layers)]
    for j in range(rank - 1):
        for l in range(layers):
            a = sides[l]
            pivot = a[j : j + 1, :]
            column = a[:, j : j + 1]
            scale = jnp.where(ri[:, 0:1] > j, column / a[j : j + 1, j : j + 1], 0.0)
            sides[l] = a - scale * pivot
    inverses = []
    for a in sides:
        diagonal = jnp.sum(jnp.where(ri == ci, a, 0.0), axis=1, keepdims=True)
        inverses.append(a[:, rank : 2 * rank] * lax.rsqrt(diagonal))

    for l in range(layers):
        p = dot(left[l], inverses[l], NT, precision=HIGHEST)
        p_rows[l] = p
        wide_out[l] = wide_left(dot(p, inverses[l], precision=HIGHEST))
        share = rows // (xs * ys)
        p_new[l] = p_rows[l, pl.ds(pl.multiple_of(col * share, 8), share), :]
        q_new[l] = dot(inverses[l], opened(qg[1, l, row]), precision=HIGHEST)
    for copy in sent:
        copy.wait_send()
    sent.clear()
    for l in range(layers):
        pass_on(1, l)
    for l in range(layers):
        all_passed(1, l)
        right_out[l] = q_columns(1, l)
    for copy in sent:
        copy.wait_send()


def error_kernel(merged, wide, right, p_in, q_in, p_new, q_new, error, buf, tall, out_sem, small_sem):
    layers, rows, cols = buf.shape
    step = 128
    small = [
        pltpu.make_async_copy(p_in, p_new, small_sem.at[0]),
        pltpu.make_async_copy(q_in, q_new, small_sem.at[1]),
    ]
    for c in small:
        c.start()
    outs = []
    for l in range(layers):
        tall[...] = tall_right(right[l])
        for i in range(rows // step):
            at = pl.ds(i * step, step)
            buf[l, at, :] = merged[l, at, :] - dot(wide[l, at, :], tall[...])
            copy = pltpu.make_async_copy(buf.at[l, at, :], error.at[l, at, :], out_sem.at[l, i])
            copy.start()
            outs.append(copy)
    for c in outs + small:
        c.wait()


def shards(xs, ys, zs, grad, memory, p_prev, q_prev):
    layers, rows, cols = grad.shape
    rank = p_prev.shape[2]
    wire = 24
    dma = pltpu.SemaphoreType.DMA
    hbm = pl.BlockSpec(memory_space=pltpu.HBM)
    vmem = pl.BlockSpec(memory_space=pltpu.VMEM)
    block = rows // 8

    def body(*refs):
        factor_kernel(zs, xs, ys, *refs)

    merged, wide, right, p_new, q_new = pl.pallas_call(
        body,
        out_shape=(
            jax.ShapeDtypeStruct((layers, rows, cols), F32),
            jax.ShapeDtypeStruct((layers, rows, 6 * rank), BF16),
            jax.ShapeDtypeStruct((layers, rank, cols), F32),
            jax.ShapeDtypeStruct(p_prev.shape, F32),
            jax.ShapeDtypeStruct(q_prev.shape, F32),
        ),
        in_specs=[hbm] * 4,
        out_specs=(vmem,) * 5,
        scratch_shapes=[
            pltpu.VMEM(q_prev.shape, F32),
            pltpu.VMEM(p_prev.shape, F32),
            pltpu.VMEM((layers, rows, cols), BF16),
            pltpu.VMEM((layers, rows, cols), BF16),
            pltpu.VMEM((layers, rows, cols), BF16),
            pltpu.VMEM((2, layers, 2 * zs, wire, 128), F32),
            pltpu.VMEM((xs, ys, layers, 8, 128), F32),
            pltpu.VMEM((layers, rows, rank), F32),
            pltpu.VMEM((layers, rows, 6 * rank), BF16),
            pltpu.VMEM((layers, 6 * rank, cols), BF16),
            pltpu.VMEM((layers, 2, 4, block, 128), F32),
            pltpu.VMEM((layers, 2, 4, block, 128), F32),
            pltpu.VMEM((layers, rows, rank), F32),
            pltpu.VMEM((layers, 2, 8, 128), F32),
            pltpu.VMEM((layers, zs, 8, 128), F32),
            pltpu.VMEM((layers, 2, zs, wire, 128), F32),
            pltpu.VMEM((layers, zs, wire, 128), F32),
            pltpu.VMEM((layers, zs, wire, 128), F32),
            pltpu.VMEM((layers, zs, wire, 128), F32),
            dma((2 + 2 * layers,)),
            dma((2, layers, zs)),
            dma((2, layers, zs)),
            dma((2, layers, zs)),
            dma((2, layers, zs)),
            dma((xs, ys)),
            dma((xs, ys)),
            dma((2, layers, 2, 4)),
            dma((2, layers, 2, 4)),
            dma((layers,)),
            dma((layers,)),
            dma((layers, zs)),
            dma((layers, zs)),
            dma((layers,)),
            dma((layers,)),
            dma((layers, zs)),
            dma((layers, zs)),
        ],
        compiler_params=pltpu.CompilerParams(
            collective_id=0, has_side_effects=True, vmem_limit_bytes=28 * 1024 * 1024
        ),
        name="factors",
    )(*(pltpu.with_memory_space_constraint(v, pltpu.HBM) for v in (grad, memory, p_prev, q_prev)))
    return pl.pallas_call(
        error_kernel,
        out_shape=(
            jax.ShapeDtypeStruct(p_prev.shape, F32),
            jax.ShapeDtypeStruct(q_prev.shape, F32),
            jax.ShapeDtypeStruct((layers, rows, cols), F32),
        ),
        in_specs=[vmem] * 5,
        out_specs=(hbm,) * 3,
        scratch_shapes=[
            pltpu.VMEM((layers, rows, cols), F32),
            pltpu.VMEM((6 * rank, cols), BF16),
            dma((layers, rows // 128)),
            dma((2,)),
        ],
        compiler_params=pltpu.CompilerParams(vmem_limit_bytes=32 * 1024 * 1024),
        name="error",
    )(merged, wide, right, p_new, q_new)


def solution(mesh):
    placed = (
        P(None, "row", "col"),
        P(None, "row", "col"),
        P(None, ("row", "col"), None),
        P(None, ("col", "row"), None),
    )
    xs = ys = 4
    zs = mesh.shape["row"] // 2

    def body(grad, memory, p_prev, q_prev):
        p_new, q_new, error = shards(xs, ys, zs, grad, memory, p_prev, jnp.swapaxes(q_prev, 1, 2))
        return p_new, jnp.swapaxes(q_new, 1, 2), error

    return jax.shard_map(
        body,
        mesh=mesh,
        in_specs=placed,
        out_specs=(
            P(None, ("row", "col"), None),
            P(None, ("col", "row"), None),
            P(None, "row", "col"),
        ),
        check_vma=False,
    )
```

```python
import jax
import jax.numpy as jnp
from jax import lax
from jax.experimental import pallas as pl
from jax.experimental.pallas import tpu as pltpu
from jax.sharding import PartitionSpec as P

F32, BF16 = jnp.float32, jnp.bfloat16
NT = (((1,), (1,)), ((), ()))
NN = (((1,), (0,)), ((), ()))
MESH = pl.DeviceIdType.MESH


def dot(a, b, dims=NN):
    return lax.dot_general(a, b, dims, preferred_element_type=F32)


def pieces(v):
    first = v.astype(BF16).astype(F32)
    rest = v - first
    second = rest.astype(BF16).astype(F32)
    return first, second, rest - second


def shut(s):
    n = s.shape[1]
    low = jnp.concatenate([s[24:32, i * 32 : i * 32 + 32] for i in range(n // 32)], axis=0)
    return jnp.concatenate([s[0:24], low], axis=1)


def opened(p):
    low = jnp.concatenate([p[8 * i : 8 * i + 8, 96:128] for i in range(3)], axis=1)
    return jnp.concatenate([p[:, 0:96], low], axis=0)


def wide_left(p):
    a, b, c = pieces(p)
    return jnp.concatenate([a, a, a, b, b, c], axis=1).astype(BF16)


def tall_right(q):
    a, b, c = (v.astype(BF16) for v in pieces(q))
    return jnp.concatenate([a, b, c, a, b, a], axis=0)


def wide_right(q):
    a, b, c = pieces(q)
    return jnp.concatenate([a, b, c, a, b, a], axis=1).astype(BF16)


def folded(v):
    v = v[0:32] + v[32:64] + v[64:96]
    return v[:, 0:32] + v[:, 32:64] + v[:, 64:96]


def inverse_factors(grams):
    n, panel = grams[0].shape[0], 8
    ri = lax.broadcasted_iota(jnp.int32, (n, 2 * n), 0)
    ci = lax.broadcasted_iota(jnp.int32, (n, 2 * n), 1)
    eye = jnp.where(ri[:, 0:n] == ci[:, 0:n], 1.0, 0.0).astype(F32)
    sides = [jnp.concatenate([g, eye], axis=1) for g in grams]
    roots = [jnp.zeros((n, 2 * n), F32) for g in grams]
    for first in range(0, n, panel):
        columns = [
            [jnp.broadcast_to(a[:, first + k : first + k + 1], (n, 2 * n)) for k in range(panel)] for a in sides
        ]
        for k in range(panel):
            j = first + k
            for i in range(len(sides)):
                own = columns[i][k]
                pivot = own[j : j + 1, :]
                roots[i] = jnp.where(ri == j, pivot, roots[i])
                scale = jnp.where(ri > j, own * (1.0 / pivot), 0.0)
                for other in range(k + 1, panel):
                    columns[i][other] = columns[i][other] - scale * columns[i][other][j : j + 1, :]
                sides[i] = sides[i] - scale * sides[i][j : j + 1, :]
    return [(a * lax.rsqrt(r))[:, n : 2 * n] for a, r in zip(sides, roots)]


def factor_kernel(
    zs, xs, ys,
    grad, memory, p_prev, q_prev,
    tile, wide_out, right_out, p_new, q_new,
    q_in, p_in, gbuf, split, qg, pg, p_rows, wide, tall, b1, b2, left, gd, gz, rb, rd, rs, rr,
    load_sem, zq_send, zq_recv, dq_send, dq_recv, p_send, p_recv, b_send, b_recv,
    gd_send, gd_recv, gz_send, gz_recv, rd_send, rd_recv, rz_send, rz_recv,
):
    layers, rows, cols = tile.shape
    row, col = lax.axis_index("row"), lax.axis_index("col")
    z, core = row // 2, row % 2
    x, y = col // ys, col % ys
    partner = {"row": z * 2 + (1 - core)}

    def z_peer(d):
        return {"row": ((z + d) % zs) * 2 + core}

    def xy_peer(dx, dy):
        return {"col": lax.rem(x + dx, xs) * ys + lax.rem(y + dy, ys)}

    def x_peer(d):
        return {"col": ((x + d) % xs) * ys + y}

    def y_peer(d):
        return {"col": x * ys + (y + d) % ys}

    def remote(src, dst, send, recv, device):
        return pltpu.make_async_remote_copy(
            src_ref=src, dst_ref=dst, send_sem=send, recv_sem=recv, device_id=device, device_id_type=MESH
        )

    sent = []

    def start(copy):
        copy.start()
        sent.append(copy)
        return copy

    load_q = pltpu.make_async_copy(q_prev, q_in, load_sem.at[0])
    load_p = pltpu.make_async_copy(p_prev, p_in, load_sem.at[1])
    load_q.start()
    load_p.start()
    loads = []
    for l in range(layers):
        pair = (
            pltpu.make_async_copy(memory.at[l], tile.at[l], load_sem.at[2 + 2 * l]),
            pltpu.make_async_copy(grad.at[l], gbuf.at[l], load_sem.at[3 + 2 * l]),
        )
        for c in pair:
            c.start()
        loads.append(pair)

    barrier = pltpu.get_barrier_semaphore()
    peers = [partner] + [z_peer(d) for d in range(1, zs)]
    offsets = [(dx, dy) for dx in (2, 1, 3, 0) for dy in (2, 1, 3, 0) if dx or dy]
    peers += [xy_peer(dx, dy) for dx, dy in offsets]
    for device in peers:
        pl.semaphore_signal(barrier, inc=1, device_id=device, device_id_type=MESH)

    load_q.wait()
    for l in range(layers):
        qg[0, row, l] = shut(q_in[l])
    load_p.wait()
    for l in range(layers):
        p = p_in[l]
        pg[x, y, l] = jnp.concatenate([p[0:8], p[8:16], p[16:24], jnp.zeros((8, 32), F32)], axis=1)
    for l in range(layers):
        for c in loads[l]:
            c.wait()

        @pl.loop(0, rows // 32)
        def _(i):
            at = pl.ds(pl.multiple_of(i * 32, 32), 32)
            t = gbuf[l, at, :].astype(F32) + tile[l, at, :]
            tile[l, at, :] = t
            t1 = t.astype(BF16)
            split[l, at, :] = t1
            split[l, pl.ds(pl.multiple_of(rows + i * 32, 32), 32), :] = (t - t1.astype(F32)).astype(BF16)

    pl.semaphore_wait(barrier, len(peers))

    far_first = sorted(range(1, zs), key=lambda d: -min(d, zs - d))
    near_first = far_first[::-1]

    def shard(phase, l, slot):
        return qg.at[phase, slot] if l is None else qg.at[phase, slot, l]

    def send_shards(phase, l=None):
        mine, i = shard(phase, l, row), l or 0
        for d in far_first:
            start(remote(mine, mine, zq_send.at[phase, i, d], zq_recv.at[phase, i, d], z_peer(d)))
        start(remote(mine, mine, dq_send.at[phase, i, 0], dq_recv.at[phase, i, 0], partner))

    def pass_on(phase, l=None):
        i = l or 0
        for d in near_first:
            there = shard(phase, l, lax.rem(z + zs - d, zs) * 2 + core)
            remote(there, there, zq_send.at[phase, i, d], zq_recv.at[phase, i, d], z_peer(d)).wait_recv()
            start(remote(there, there, dq_send.at[phase, i, d], dq_recv.at[phase, i, d], partner))

    def all_passed(phase, l=None):
        i = l or 0
        for d in range(zs):
            there = shard(phase, l, lax.rem(z + zs - d, zs) * 2 + (1 - core))
            remote(there, there, dq_send.at[phase, i, d], dq_recv.at[phase, i, d], partner).wait_recv()

    send_shards(0)
    for dx, dy in offsets:
        mine = pg.at[x, y]
        start(remote(mine, mine, p_send.at[dx, dy], p_recv.at[dx, dy], xy_peer(dx, dy)))

    def q_columns(phase, l):
        return jnp.concatenate([opened(qg[phase, r, l]) for r in range(2 * zs)], axis=1)

    step = 256
    half = rows // 2
    block = half // 4

    def left_part(l):
        tall[l] = tall_right(q_columns(0, l))
        wide[l] = wide_left(p_rows[l])
        q3 = tall[l, 0:96, :]
        square = dot(q3, q3, NT)
        parts = []
        for h in range(2):
            first, second = (split[l, i * rows + h * half : i * rows + (h + 1) * half, :] for i in range(2))
            acc = dot(first, q3, NT) + dot(second, q3, NT)
            parts.append(acc[:, 0:32] + acc[:, 32:64] + acc[:, 64:96])
        less = dot(wide[l], tall_right(folded(square)))
        return jnp.concatenate(parts, axis=0) - less

    def merge(l):
        for j in range(cols // step):
            at = pl.ds(j * step, step)
            m = tile[l, :, at] - dot(wide[l], tall[l, :, at])
            tile[l, :, at] = m
            m1 = m.astype(BF16)
            split[l, 0:rows, at] = m1
            split[l, rows : 2 * rows, at] = (m - m1.astype(F32)).astype(BF16)

    def halves(v):
        for h in range(2):
            yield jnp.concatenate([v[h * half + b * block : h * half + (b + 1) * block] for b in range(4)], axis=1)

    def exchange(buf, stage, l, h, along_y):
        n, me, peer = (ys, y, y_peer) if along_y else (xs, x, x_peer)
        mine = buf.at[l, h, me]
        for d in range(1, n):
            start(remote(mine, mine, b_send.at[stage, l, h, d], b_recv.at[stage, l, h, d], peer(d)))

    def arrived(buf, stage, l, h, along_y):
        n, me, peer = (ys, y, y_peer) if along_y else (xs, x, x_peer)
        for d in range(1, n):
            there = buf.at[l, h, (me + n - d) % n]
            remote(there, there, b_send.at[stage, l, h, d], b_recv.at[stage, l, h, d], peer(d)).wait_recv()
        total = buf[l, h, 0]
        for i in range(1, n):
            total = total + buf[l, h, i]
        return total

    def first_stage(l):
        part = left_part(l)
        for h, v in enumerate(halves(part)):
            me = y if h == 0 else x
            b1[l, h, me] = v
            exchange(b1, 0, l, h, h == 0)

    def second_stage(l):
        for h in range(2):
            total = arrived(b1, 0, l, h, h == 0)
            me = x if h == 0 else y
            b2[l, h, me] = total
            exchange(b2, 1, l, h, h == 1)

    pass_on(0)
    for dx, dy in offsets[::-1]:
        there = pg.at[lax.rem(x + xs - dx, xs), lax.rem(y + ys - dy, ys)]
        remote(there, there, p_send.at[dx, dy], p_recv.at[dx, dy], xy_peer(dx, dy)).wait_recv()
    for l in range(layers):
        for c in range(xs * ys):
            v = pg[c // ys, c % ys, l]
            p_rows[l, 24 * c : 24 * c + 24, :] = jnp.concatenate([v[:, 32 * b : 32 * b + 32] for b in range(3)], axis=0)
    all_passed(0)
    first_stage(0)
    first_stage(1)
    merge(0)
    merge(1)
    second_stage(0)
    second_stage(1)

    def right_part(l):
        for h in range(2):
            total = arrived(b2, 1, l, h, h == 1)
            for b in range(4):
                left[l, h * half + b * block : h * half + (b + 1) * block, :] = total[:, 32 * b : 32 * b + 32]
        t1, t2, t3 = (t.astype(BF16) for t in pieces(left[l].T))
        lhs = jnp.concatenate([t1, t2, t3], axis=0)
        g = folded(dot(lhs, lhs, NT))
        gd[l, core] = jnp.concatenate([g[8 * i : 8 * i + 8] for i in range(4)], axis=1)
        mine = gd.at[l, core]
        start(remote(mine, mine, gd_send.at[l], gd_recv.at[l], partner))
        full = dot(lhs, split[l, 0:rows, :]) + dot(lhs, split[l, rows : 2 * rows, :])
        r = full[0:32] + full[32:64] + full[64:96]
        for s in range(2 * zs):
            rb[l, s % 2, s // 2] = shut(r[:, 96 * s : 96 * s + 96])
        start(remote(rb.at[l, 1 - core], rd.at[l], rd_send.at[l], rd_recv.at[l], partner))

    def send_gram(l):
        there = gd.at[l, 1 - core]
        remote(there, there, gd_send.at[l], gd_recv.at[l], partner).wait_recv()
        gz[l, z] = gd[l, 0] + gd[l, 1]
        mine = gz.at[l, z]
        for d in far_first:
            start(remote(mine, mine, gz_send.at[l, d], gz_recv.at[l, d], z_peer(d)))

    def scatter(l):
        remote(rb.at[l, 1 - core], rd.at[l], rd_send.at[l], rd_recv.at[l], partner).wait_recv()
        rs[l] = rb[l, core] + rd[l]
        for d in far_first:
            to = (z + d) % zs
            start(remote(rs.at[l, to], rr.at[l, z], rz_send.at[l, d], rz_recv.at[l, d], z_peer(d)))
        rr[l, z] = rs[l, z]

    right_part(0)
    send_gram(0)
    scatter(0)
    right_part(1)
    scatter(1)
    send_gram(1)

    def gather(l):
        for d in near_first:
            there = rr.at[l, (z + zs - d) % zs]
            remote(rs.at[l, 0], there, rz_send.at[l, d], rz_recv.at[l, d], z_peer(d)).wait_recv()
        total = rr[l, 0]
        for i in range(1, zs):
            total = total + rr[l, i]
        qg[1, row, l] = total
        send_shards(1, l)

    gather(0)
    gather(1)

    def whole_gram(l):
        for d in range(1, zs):
            there = gz.at[l, (z + zs - d) % zs]
            remote(there, there, gz_send.at[l, d], gz_recv.at[l, d], z_peer(d)).wait_recv()
        g = gz[l, 0]
        for i in range(1, zs):
            g = g + gz[l, i]
        return jnp.concatenate([g[:, 32 * i : 32 * i + 32] for i in range(4)], axis=0)

    for l in range(layers):
        wide[l] = wide_left(left[l])
    inverses = inverse_factors([whole_gram(l) for l in range(layers)])
    for l in range(layers):
        inverse = inverses[l]
        tall_inverse = tall_right(inverse)
        p = dot(wide[l], wide_right(inverse), NT)
        p_rows[l] = p
        wide_out[l] = wide_left(dot(wide_left(p), tall_inverse))
        share = rows // (xs * ys)
        p_new[l] = p_rows[l, pl.ds(pl.multiple_of(col * share, 8), share), :]
        q_new[l] = dot(wide_left(inverse), tall_right(opened(qg[1, row, l])))
    for copy in sent:
        copy.wait_send()
    sent.clear()
    for l in range(layers):
        pass_on(1, l)
    for l in range(layers):
        all_passed(1, l)
        right_out[l] = q_columns(1, l)
    for copy in sent:
        copy.wait_send()


def error_kernel(merged, wide, right, p_in, q_in, p_new, q_new, error, buf, tall, out_sem, small_sem):
    layers, rows, cols = buf.shape
    step = 128
    small = [
        pltpu.make_async_copy(p_in, p_new, small_sem.at[0]),
        pltpu.make_async_copy(q_in, q_new, small_sem.at[1]),
    ]
    for c in small:
        c.start()
    outs = []
    for l in range(layers):
        tall[...] = tall_right(right[l])
        for i in range(rows // step):
            at = pl.ds(i * step, step)
            buf[l, at, :] = merged[l, at, :] - dot(wide[l, at, :], tall[...])
            copy = pltpu.make_async_copy(buf.at[l, at, :], error.at[l, at, :], out_sem.at[l, i])
            copy.start()
            outs.append(copy)
    for c in outs + small:
        c.wait()


def shards(xs, ys, zs, grad, memory, p_prev, q_prev):
    layers, rows, cols = grad.shape
    rank = p_prev.shape[2]
    wire = 24
    dma = pltpu.SemaphoreType.DMA
    hbm = pl.BlockSpec(memory_space=pltpu.HBM)
    vmem = pl.BlockSpec(memory_space=pltpu.VMEM)
    block = rows // 8

    def body(*refs):
        factor_kernel(zs, xs, ys, *refs)

    merged, wide, right, p_new, q_new = pl.pallas_call(
        body,
        out_shape=(
            jax.ShapeDtypeStruct((layers, rows, cols), F32),
            jax.ShapeDtypeStruct((layers, rows, 6 * rank), BF16),
            jax.ShapeDtypeStruct((layers, rank, cols), F32),
            jax.ShapeDtypeStruct(p_prev.shape, F32),
            jax.ShapeDtypeStruct(q_prev.shape, F32),
        ),
        in_specs=[hbm] * 4,
        out_specs=(vmem,) * 5,
        scratch_shapes=[
            pltpu.VMEM(q_prev.shape, F32),
            pltpu.VMEM(p_prev.shape, F32),
            pltpu.VMEM((layers, rows, cols), BF16),
            pltpu.VMEM((layers, 2 * rows, cols), BF16),
            pltpu.VMEM((2, 2 * zs, layers, wire, 128), F32),
            pltpu.VMEM((xs, ys, layers, 8, 128), F32),
            pltpu.VMEM((layers, rows, rank), F32),
            pltpu.VMEM((layers, rows, 6 * rank), BF16),
            pltpu.VMEM((layers, 6 * rank, cols), BF16),
            pltpu.VMEM((layers, 2, 4, block, 128), F32),
            pltpu.VMEM((layers, 2, 4, block, 128), F32),
            pltpu.VMEM((layers, rows, rank), F32),
            pltpu.VMEM((layers, 2, 8, 128), F32),
            pltpu.VMEM((layers, zs, 8, 128), F32),
            pltpu.VMEM((layers, 2, zs, wire, 128), F32),
            pltpu.VMEM((layers, zs, wire, 128), F32),
            pltpu.VMEM((layers, zs, wire, 128), F32),
            pltpu.VMEM((layers, zs, wire, 128), F32),
            dma((2 + 2 * layers,)),
            dma((2, layers, zs)),
            dma((2, layers, zs)),
            dma((2, layers, zs)),
            dma((2, layers, zs)),
            dma((xs, ys)),
            dma((xs, ys)),
            dma((2, layers, 2, 4)),
            dma((2, layers, 2, 4)),
            dma((layers,)),
            dma((layers,)),
            dma((layers, zs)),
            dma((layers, zs)),
            dma((layers,)),
            dma((layers,)),
            dma((layers, zs)),
            dma((layers, zs)),
        ],
        compiler_params=pltpu.CompilerParams(
            collective_id=0, has_side_effects=True, vmem_limit_bytes=28 * 1024 * 1024
        ),
        name="factors",
    )(*(pltpu.with_memory_space_constraint(v, pltpu.HBM) for v in (grad, memory, p_prev, q_prev)))
    return pl.pallas_call(
        error_kernel,
        out_shape=(
            jax.ShapeDtypeStruct(p_prev.shape, F32),
            jax.ShapeDtypeStruct(q_prev.shape, F32),
            jax.ShapeDtypeStruct((layers, rows, cols), F32),
        ),
        in_specs=[vmem] * 5,
        out_specs=(hbm,) * 3,
        scratch_shapes=[
            pltpu.VMEM((layers, rows, cols), F32),
            pltpu.VMEM((6 * rank, cols), BF16),
            dma((layers, rows // 128)),
            dma((2,)),
        ],
        compiler_params=pltpu.CompilerParams(vmem_limit_bytes=32 * 1024 * 1024),
        name="error",
    )(merged, wide, right, p_new, q_new)


def solution(mesh):
    placed = (
        P(None, "row", "col"),
        P(None, "row", "col"),
        P(None, ("row", "col"), None),
        P(None, ("col", "row"), None),
    )
    xs = ys = 4
    zs = mesh.shape["row"] // 2

    def body(grad, memory, p_prev, q_prev):
        p_new, q_new, error = shards(xs, ys, zs, grad, memory, p_prev, jnp.swapaxes(q_prev, 1, 2))
        return p_new, jnp.swapaxes(q_new, 1, 2), error

    return jax.shard_map(
        body,
        mesh=mesh,
        in_specs=placed,
        out_specs=(
            P(None, ("row", "col"), None),
            P(None, ("col", "row"), None),
            P(None, "row", "col"),
        ),
        check_vma=False,
    )
```

```python
import jax
import jax.numpy as jnp
from jax import lax
from jax.experimental import pallas as pl
from jax.experimental.pallas import tpu as pltpu
from jax.sharding import PartitionSpec as P

F32, BF16 = jnp.float32, jnp.bfloat16
NT = (((1,), (1,)), ((), ()))
NN = (((1,), (0,)), ((), ()))
MESH = pl.DeviceIdType.MESH


def dot(a, b, dims=NN):
    return lax.dot_general(a, b, dims, preferred_element_type=F32)


def pieces(v):
    first = v.astype(BF16).astype(F32)
    rest = v - first
    second = rest.astype(BF16).astype(F32)
    return first, second, rest - second


def shut(s):
    n = s.shape[1]
    low = jnp.concatenate([s[24:32, i * 32 : i * 32 + 32] for i in range(n // 32)], axis=0)
    return jnp.concatenate([s[0:24], low], axis=1)


def opened(p):
    low = jnp.concatenate([p[8 * i : 8 * i + 8, 96:128] for i in range(3)], axis=1)
    return jnp.concatenate([p[:, 0:96], low], axis=0)


def wide_left(p):
    a, b, c = pieces(p)
    return jnp.concatenate([a, a, a, b, b, c], axis=1).astype(BF16)


def tall_right(q):
    a, b, c = (v.astype(BF16) for v in pieces(q))
    return jnp.concatenate([a, b, c, a, b, a], axis=0)


def wide_right(q):
    a, b, c = pieces(q)
    return jnp.concatenate([a, b, c, a, b, a], axis=1).astype(BF16)


def folded(v):
    v = v[0:32] + v[32:64] + v[64:96]
    return v[:, 0:32] + v[:, 32:64] + v[:, 64:96]


def inverse_factors(grams):
    n, panel = grams[0].shape[0], 8
    ri = lax.broadcasted_iota(jnp.int32, (n, 2 * n), 0)
    ci = lax.broadcasted_iota(jnp.int32, (n, 2 * n), 1)
    eye = jnp.where(ri[:, 0:n] == ci[:, 0:n], 1.0, 0.0).astype(F32)
    sides = [jnp.concatenate([g, eye], axis=1) for g in grams]
    roots = [jnp.zeros((n, 2 * n), F32) for g in grams]
    for first in range(0, n, panel):
        columns = [
            [jnp.broadcast_to(a[:, first + k : first + k + 1], (n, 2 * n)) for k in range(panel)] for a in sides
        ]
        for k in range(panel):
            j = first + k
            for i in range(len(sides)):
                own = columns[i][k]
                pivot = own[j : j + 1, :]
                roots[i] = jnp.where(ri == j, pivot, roots[i])
                scale = jnp.where(ri > j, own * (1.0 / pivot), 0.0)
                for other in range(k + 1, panel):
                    columns[i][other] = columns[i][other] - scale * columns[i][other][j : j + 1, :]
                sides[i] = sides[i] - scale * sides[i][j : j + 1, :]
    return [(a * lax.rsqrt(r))[:, n : 2 * n] for a, r in zip(sides, roots)]


def factor_kernel(
    zs, xs, ys,
    grad, memory, p_prev, q_prev,
    tile, wide_out, right_out, p_new, q_new,
    q_in, p_in, gbuf, split, qg, pg, p_rows, wide, tall, b1, b2, left, gd, gz, rb, rd, rs, rr,
    load_sem, zq_send, zq_recv, dq_send, dq_recv, p_send, p_recv, b_send, b_recv,
    gd_send, gd_recv, gz_send, gz_recv, rd_send, rd_recv, rz_send, rz_recv,
):
    layers, rows, cols = tile.shape
    row, col = lax.axis_index("row"), lax.axis_index("col")
    z, core = row // 2, row % 2
    x, y = col // ys, col % ys
    partner = {"row": z * 2 + (1 - core)}

    def z_peer(d):
        return {"row": ((z + d) % zs) * 2 + core}

    def xy_peer(dx, dy):
        return {"col": lax.rem(x + dx, xs) * ys + lax.rem(y + dy, ys)}

    def x_peer(d):
        return {"col": ((x + d) % xs) * ys + y}

    def y_peer(d):
        return {"col": x * ys + (y + d) % ys}

    def remote(src, dst, send, recv, device):
        return pltpu.make_async_remote_copy(
            src_ref=src, dst_ref=dst, send_sem=send, recv_sem=recv, device_id=device, device_id_type=MESH
        )

    sent = []

    def start(copy):
        copy.start()
        sent.append(copy)
        return copy

    load_q = pltpu.make_async_copy(q_prev, q_in, load_sem.at[0])
    load_p = pltpu.make_async_copy(p_prev, p_in, load_sem.at[1])
    load_q.start()
    load_p.start()
    loads = []
    for l in range(layers):
        pair = (
            pltpu.make_async_copy(memory.at[l], tile.at[l], load_sem.at[2 + 2 * l]),
            pltpu.make_async_copy(grad.at[l], gbuf.at[l], load_sem.at[3 + 2 * l]),
        )
        for c in pair:
            c.start()
        loads.append(pair)

    barrier = pltpu.get_barrier_semaphore()
    peers = [partner] + [z_peer(d) for d in range(1, zs)]
    offsets = [(dx, dy) for dx in (2, 1, 3, 0) for dy in (2, 1, 3, 0) if dx or dy]
    peers += [xy_peer(dx, dy) for dx, dy in offsets]
    for device in peers:
        pl.semaphore_signal(barrier, inc=1, device_id=device, device_id_type=MESH)

    load_q.wait()
    for l in range(layers):
        qg[0, row, l] = shut(q_in[l])
    load_p.wait()
    for l in range(layers):
        p = p_in[l]
        pg[x, y, l] = jnp.concatenate([p[0:8], p[8:16], p[16:24], jnp.zeros((8, 32), F32)], axis=1)
    for l in range(layers):
        for c in loads[l]:
            c.wait()

        @pl.loop(0, rows // 32)
        def _(i):
            at = pl.ds(pl.multiple_of(i * 32, 32), 32)
            t = gbuf[l, at, :].astype(F32) + tile[l, at, :]
            tile[l, at, :] = t
            t1 = t.astype(BF16)
            split[l, at, :] = t1
            split[l, pl.ds(pl.multiple_of(rows + i * 32, 32), 32), :] = (t - t1.astype(F32)).astype(BF16)

    pl.semaphore_wait(barrier, len(peers))

    far_first = sorted(range(1, zs), key=lambda d: -min(d, zs - d))
    near_first = far_first[::-1]

    def shard(phase, l, slot):
        return qg.at[phase, slot] if l is None else qg.at[phase, slot, l]

    def send_shards(phase, l=None):
        mine, i = shard(phase, l, row), l or 0
        for d in far_first:
            start(remote(mine, mine, zq_send.at[phase, i, d], zq_recv.at[phase, i, d], z_peer(d)))
        start(remote(mine, mine, dq_send.at[phase, i, 0], dq_recv.at[phase, i, 0], partner))

    def pass_on(phase, l=None):
        i = l or 0
        for d in near_first:
            there = shard(phase, l, lax.rem(z + zs - d, zs) * 2 + core)
            remote(there, there, zq_send.at[phase, i, d], zq_recv.at[phase, i, d], z_peer(d)).wait_recv()
            start(remote(there, there, dq_send.at[phase, i, d], dq_recv.at[phase, i, d], partner))

    def all_passed(phase, l=None):
        i = l or 0
        for d in range(zs):
            there = shard(phase, l, lax.rem(z + zs - d, zs) * 2 + (1 - core))
            remote(there, there, dq_send.at[phase, i, d], dq_recv.at[phase, i, d], partner).wait_recv()

    send_shards(0)
    for dx, dy in offsets:
        mine = pg.at[x, y]
        start(remote(mine, mine, p_send.at[dx, dy], p_recv.at[dx, dy], xy_peer(dx, dy)))

    def q_columns(phase, l):
        return jnp.concatenate([opened(qg[phase, r, l]) for r in range(2 * zs)], axis=1)

    step = 256
    half = rows // 2
    block = half // 4

    def left_part(l):
        tall[l] = tall_right(q_columns(0, l))
        wide[l] = wide_left(p_rows[l])
        q3 = tall[l, 0:96, :]
        square = dot(q3, q3, NT)
        parts = []
        for h in range(2):
            first, second = (split[l, i * rows + h * half : i * rows + (h + 1) * half, :] for i in range(2))
            acc = dot(first, q3, NT) + dot(second, q3, NT)
            parts.append(acc[:, 0:32] + acc[:, 32:64] + acc[:, 64:96])
        less = dot(wide[l], tall_right(folded(square)))
        return jnp.concatenate(parts, axis=0) - less

    def merge(l):
        for j in range(cols // step):
            at = pl.ds(j * step, step)
            m = tile[l, :, at] - dot(wide[l], tall[l, :, at])
            tile[l, :, at] = m
            m1 = m.astype(BF16)
            split[l, 0:rows, at] = m1
            split[l, rows : 2 * rows, at] = (m - m1.astype(F32)).astype(BF16)

    def halves(v):
        for h in range(2):
            yield jnp.concatenate([v[h * half + b * block : h * half + (b + 1) * block] for b in range(4)], axis=1)

    def exchange(buf, stage, l, h, along_y):
        n, me, peer = (ys, y, y_peer) if along_y else (xs, x, x_peer)
        mine = buf.at[l, h, me]
        for d in range(1, n):
            start(remote(mine, mine, b_send.at[stage, l, h, d], b_recv.at[stage, l, h, d], peer(d)))

    def arrived(buf, stage, l, h, along_y):
        n, me, peer = (ys, y, y_peer) if along_y else (xs, x, x_peer)
        for d in range(1, n):
            there = buf.at[l, h, (me + n - d) % n]
            remote(there, there, b_send.at[stage, l, h, d], b_recv.at[stage, l, h, d], peer(d)).wait_recv()
        total = buf[l, h, 0]
        for i in range(1, n):
            total = total + buf[l, h, i]
        return total

    def first_stage(l):
        part = left_part(l)
        for h, v in enumerate(halves(part)):
            me = y if h == 0 else x
            b1[l, h, me] = v
            exchange(b1, 0, l, h, h == 0)

    def second_stage(l):
        for h in range(2):
            total = arrived(b1, 0, l, h, h == 0)
            me = x if h == 0 else y
            b2[l, h, me] = total
            exchange(b2, 1, l, h, h == 1)

    pass_on(0)
    for dx, dy in offsets[::-1]:
        there = pg.at[lax.rem(x + xs - dx, xs), lax.rem(y + ys - dy, ys)]
        remote(there, there, p_send.at[dx, dy], p_recv.at[dx, dy], xy_peer(dx, dy)).wait_recv()
    for l in range(layers):
        for c in range(xs * ys):
            v = pg[c // ys, c % ys, l]
            p_rows[l, 24 * c : 24 * c + 24, :] = jnp.concatenate([v[:, 32 * b : 32 * b + 32] for b in range(3)], axis=0)
    all_passed(0)
    first_stage(0)
    first_stage(1)
    merge(0)
    merge(1)
    second_stage(0)
    second_stage(1)

    def right_part(l):
        for h in range(2):
            total = arrived(b2, 1, l, h, h == 1)
            for b in range(4):
                left[l, h * half + b * block : h * half + (b + 1) * block, :] = total[:, 32 * b : 32 * b + 32]
        t1, t2, t3 = (t.astype(BF16) for t in pieces(left[l].T))
        lhs = jnp.concatenate([t1, t2, t3], axis=0)
        g = folded(dot(lhs, lhs, NT))
        gd[l, core] = jnp.concatenate([g[8 * i : 8 * i + 8] for i in range(4)], axis=1)
        mine = gd.at[l, core]
        start(remote(mine, mine, gd_send.at[l], gd_recv.at[l], partner))
        full = dot(lhs, split[l, 0:rows, :]) + dot(lhs, split[l, rows : 2 * rows, :])
        r = full[0:32] + full[32:64] + full[64:96]
        for s in range(2 * zs):
            rb[l, s % 2, s // 2] = shut(r[:, 96 * s : 96 * s + 96])
        start(remote(rb.at[l, 1 - core], rd.at[l], rd_send.at[l], rd_recv.at[l], partner))

    def send_gram(l):
        there = gd.at[l, 1 - core]
        remote(there, there, gd_send.at[l], gd_recv.at[l], partner).wait_recv()
        gz[l, z] = gd[l, 0] + gd[l, 1]
        mine = gz.at[l, z]
        for d in far_first:
            start(remote(mine, mine, gz_send.at[l, d], gz_recv.at[l, d], z_peer(d)))

    def scatter(l):
        remote(rb.at[l, 1 - core], rd.at[l], rd_send.at[l], rd_recv.at[l], partner).wait_recv()
        rs[l] = rb[l, core] + rd[l]
        for d in far_first:
            to = (z + d) % zs
            start(remote(rs.at[l, to], rr.at[l, z], rz_send.at[l, d], rz_recv.at[l, d], z_peer(d)))
        rr[l, z] = rs[l, z]

    right_part(0)
    send_gram(0)
    scatter(0)
    right_part(1)
    scatter(1)
    send_gram(1)

    def gather(l):
        for d in near_first:
            there = rr.at[l, (z + zs - d) % zs]
            remote(rs.at[l, 0], there, rz_send.at[l, d], rz_recv.at[l, d], z_peer(d)).wait_recv()
        total = rr[l, 0]
        for i in range(1, zs):
            total = total + rr[l, i]
        qg[1, row, l] = total
        send_shards(1, l)

    gather(0)
    gather(1)

    def whole_gram(l):
        for d in range(1, zs):
            there = gz.at[l, (z + zs - d) % zs]
            remote(there, there, gz_send.at[l, d], gz_recv.at[l, d], z_peer(d)).wait_recv()
        g = gz[l, 0]
        for i in range(1, zs):
            g = g + gz[l, i]
        return jnp.concatenate([g[:, 32 * i : 32 * i + 32] for i in range(4)], axis=0)

    for l in range(layers):
        wide[l] = wide_left(left[l])
    inverses = inverse_factors([whole_gram(l) for l in range(layers)])
    for l in range(layers):
        inverse = inverses[l]
        tall_inverse = tall_right(inverse)
        p = dot(wide[l], wide_right(inverse), NT)
        p_rows[l] = p
        side = wide_out if l else wide.at[0]
        side[...] = wide_left(dot(wide_left(p), tall_inverse))
        share = rows // (xs * ys)
        p_new[l] = p_rows[l, pl.ds(pl.multiple_of(col * share, 8), share), :]
        q_new[l] = dot(wide_left(inverse), tall_right(opened(qg[1, row, l])))
    for copy in sent:
        copy.wait_send()
    sent.clear()
    for l in range(layers):
        pass_on(1, l)
    all_passed(1, 0)
    tall[0] = tall_right(q_columns(1, 0))
    for j in range(cols // step):
        at = pl.ds(j * step, step)
        tile[0, :, at] = tile[0, :, at] - dot(wide[0], tall[0, :, at])
    all_passed(1, 1)
    right_out[...] = q_columns(1, 1)
    for copy in sent:
        copy.wait_send()


def error_kernel(merged, wide, right, p_in, q_in, p_new, q_new, error, buf, tall, out_sem, small_sem):
    rows, cols = buf.shape
    step = rows // 3
    copies = [pltpu.make_async_copy(merged.at[0], error.at[0], small_sem.at[2])]
    copies += [
        pltpu.make_async_copy(p_in, p_new, small_sem.at[0]),
        pltpu.make_async_copy(q_in, q_new, small_sem.at[1]),
    ]
    for c in copies:
        c.start()
    tall[...] = tall_right(right[...])
    for i in range(3):
        at = pl.ds(i * step, step)
        buf[at, :] = merged[1, at, :] - dot(wide[at, :], tall[...])
        copy = pltpu.make_async_copy(buf.at[at, :], error.at[1, at, :], out_sem.at[i])
        copy.start()
        copies.append(copy)
    for c in copies:
        c.wait()


def shards(xs, ys, zs, grad, memory, p_prev, q_prev):
    layers, rows, cols = grad.shape
    rank = p_prev.shape[2]
    wire = 24
    dma = pltpu.SemaphoreType.DMA
    hbm = pl.BlockSpec(memory_space=pltpu.HBM)
    vmem = pl.BlockSpec(memory_space=pltpu.VMEM)
    block = rows // 8

    def body(*refs):
        factor_kernel(zs, xs, ys, *refs)

    merged, wide, right, p_new, q_new = pl.pallas_call(
        body,
        out_shape=(
            jax.ShapeDtypeStruct((layers, rows, cols), F32),
            jax.ShapeDtypeStruct((rows, 6 * rank), BF16),
            jax.ShapeDtypeStruct((rank, cols), F32),
            jax.ShapeDtypeStruct(p_prev.shape, F32),
            jax.ShapeDtypeStruct(q_prev.shape, F32),
        ),
        in_specs=[hbm] * 4,
        out_specs=(vmem,) * 5,
        scratch_shapes=[
            pltpu.VMEM(q_prev.shape, F32),
            pltpu.VMEM(p_prev.shape, F32),
            pltpu.VMEM((layers, rows, cols), BF16),
            pltpu.VMEM((layers, 2 * rows, cols), BF16),
            pltpu.VMEM((2, 2 * zs, layers, wire, 128), F32),
            pltpu.VMEM((xs, ys, layers, 8, 128), F32),
            pltpu.VMEM((layers, rows, rank), F32),
            pltpu.VMEM((layers, rows, 6 * rank), BF16),
            pltpu.VMEM((layers, 6 * rank, cols), BF16),
            pltpu.VMEM((layers, 2, 4, block, 128), F32),
            pltpu.VMEM((layers, 2, 4, block, 128), F32),
            pltpu.VMEM((layers, rows, rank), F32),
            pltpu.VMEM((layers, 2, 8, 128), F32),
            pltpu.VMEM((layers, zs, 8, 128), F32),
            pltpu.VMEM((layers, 2, zs, wire, 128), F32),
            pltpu.VMEM((layers, zs, wire, 128), F32),
            pltpu.VMEM((layers, zs, wire, 128), F32),
            pltpu.VMEM((layers, zs, wire, 128), F32),
            dma((2 + 2 * layers,)),
            dma((2, layers, zs)),
            dma((2, layers, zs)),
            dma((2, layers, zs)),
            dma((2, layers, zs)),
            dma((xs, ys)),
            dma((xs, ys)),
            dma((2, layers, 2, 4)),
            dma((2, layers, 2, 4)),
            dma((layers,)),
            dma((layers,)),
            dma((layers, zs)),
            dma((layers, zs)),
            dma((layers,)),
            dma((layers,)),
            dma((layers, zs)),
            dma((layers, zs)),
        ],
        compiler_params=pltpu.CompilerParams(
            collective_id=0, has_side_effects=True, vmem_limit_bytes=28 * 1024 * 1024
        ),
        name="factors",
    )(*(pltpu.with_memory_space_constraint(v, pltpu.HBM) for v in (grad, memory, p_prev, q_prev)))
    return pl.pallas_call(
        error_kernel,
        out_shape=(
            jax.ShapeDtypeStruct(p_prev.shape, F32),
            jax.ShapeDtypeStruct(q_prev.shape, F32),
            jax.ShapeDtypeStruct((layers, rows, cols), F32),
        ),
        in_specs=[vmem] * 5,
        out_specs=(hbm,) * 3,
        scratch_shapes=[
            pltpu.VMEM((rows, cols), F32),
            pltpu.VMEM((6 * rank, cols), BF16),
            dma((3,)),
            dma((3,)),
        ],
        compiler_params=pltpu.CompilerParams(vmem_limit_bytes=32 * 1024 * 1024),
        name="error",
    )(merged, wide, right, p_new, q_new)


def solution(mesh):
    placed = (
        P(None, "row", "col"),
        P(None, "row", "col"),
        P(None, ("row", "col"), None),
        P(None, ("col", "row"), None),
    )
    xs = ys = 4
    zs = mesh.shape["row"] // 2

    def body(grad, memory, p_prev, q_prev):
        p_new, q_new, error = shards(xs, ys, zs, grad, memory, p_prev, jnp.swapaxes(q_prev, 1, 2))
        return p_new, jnp.swapaxes(q_new, 1, 2), error

    return jax.shard_map(
        body,
        mesh=mesh,
        in_specs=placed,
        out_specs=(
            P(None, ("row", "col"), None),
            P(None, ("col", "row"), None),
            P(None, "row", "col"),
        ),
        check_vma=False,
    )
```

```python
import jax
import jax.numpy as jnp
from jax import lax
from jax.experimental import pallas as pl
from jax.experimental.pallas import tpu as pltpu
from jax.sharding import PartitionSpec as P

F32, BF16 = jnp.float32, jnp.bfloat16
NT = (((1,), (1,)), ((), ()))
NN = (((1,), (0,)), ((), ()))
MESH = pl.DeviceIdType.MESH


def dot(a, b, dims=NN):
    return lax.dot_general(a, b, dims, preferred_element_type=F32)


def pieces(v):
    first = v.astype(BF16).astype(F32)
    rest = v - first
    second = rest.astype(BF16).astype(F32)
    return first, second, rest - second


def shut(s):
    n = s.shape[1]
    low = jnp.concatenate([s[24:32, i * 32 : i * 32 + 32] for i in range(n // 32)], axis=0)
    return jnp.concatenate([s[0:24], low], axis=1)


def opened(p):
    low = jnp.concatenate([p[8 * i : 8 * i + 8, 96:128] for i in range(3)], axis=1)
    return jnp.concatenate([p[:, 0:96], low], axis=0)


def wide_left(p):
    a, b, c = pieces(p)
    return jnp.concatenate([a, a, a, b, b, c], axis=1).astype(BF16)


def tall_right(q):
    a, b, c = (v.astype(BF16) for v in pieces(q))
    return jnp.concatenate([a, b, c, a, b, a], axis=0)


def wide_right(q):
    a, b, c = pieces(q)
    return jnp.concatenate([a, b, c, a, b, a], axis=1).astype(BF16)


def folded(v):
    v = v[0:32] + v[32:64] + v[64:96]
    return v[:, 0:32] + v[:, 32:64] + v[:, 64:96]


def inverse_factors(grams):
    n, panel = grams[0].shape[0], 8
    ri = lax.broadcasted_iota(jnp.int32, (n, 2 * n), 0)
    ci = lax.broadcasted_iota(jnp.int32, (n, 2 * n), 1)
    eye = jnp.where(ri[:, 0:n] == ci[:, 0:n], 1.0, 0.0).astype(F32)
    sides = [jnp.concatenate([g, eye], axis=1) for g in grams]
    roots = [jnp.zeros((n, 2 * n), F32) for g in grams]
    for first in range(0, n, panel):
        columns = [
            [jnp.broadcast_to(a[:, first + k : first + k + 1], (n, 2 * n)) for k in range(panel)] for a in sides
        ]
        for k in range(panel):
            j = first + k
            for i in range(len(sides)):
                own = columns[i][k]
                pivot = own[j : j + 1, :]
                roots[i] = jnp.where(ri == j, pivot, roots[i])
                scale = jnp.where(ri > j, own * (1.0 / pivot), 0.0)
                for other in range(k + 1, panel):
                    columns[i][other] = columns[i][other] - scale * columns[i][other][j : j + 1, :]
                sides[i] = sides[i] - scale * sides[i][j : j + 1, :]
    return [(a * lax.rsqrt(r))[:, n : 2 * n] for a, r in zip(sides, roots)]


def factor_kernel(
    zs, xs, ys,
    grad, memory, p_prev, q_prev,
    tile, wide_out, right_out, p_new, q_new,
    q_in, p_in, gbuf, split, qg, pg, p_rows, wide, tall, b1, b2, left, gd, gz, rb, rd, rs, rr,
    load_sem, zq_send, zq_recv, dq_send, dq_recv, p_send, p_recv, b_send, b_recv,
    gd_send, gd_recv, gz_send, gz_recv, rd_send, rd_recv, rz_send, rz_recv,
):
    layers, rows, cols = tile.shape
    row, col = lax.axis_index("row"), lax.axis_index("col")
    z, core = row // 2, row % 2
    x, y = col // ys, col % ys
    partner = {"row": z * 2 + (1 - core)}

    def z_peer(d):
        return {"row": ((z + d) % zs) * 2 + core}

    def xy_peer(dx, dy):
        return {"col": lax.rem(x + dx, xs) * ys + lax.rem(y + dy, ys)}

    def x_peer(d):
        return {"col": ((x + d) % xs) * ys + y}

    def y_peer(d):
        return {"col": x * ys + (y + d) % ys}

    def remote(src, dst, send, recv, device):
        return pltpu.make_async_remote_copy(
            src_ref=src, dst_ref=dst, send_sem=send, recv_sem=recv, device_id=device, device_id_type=MESH
        )

    sent = []

    def start(copy):
        copy.start()
        sent.append(copy)
        return copy

    load_q = pltpu.make_async_copy(q_prev, q_in, load_sem.at[0])
    load_p = pltpu.make_async_copy(p_prev, p_in, load_sem.at[1])
    load_q.start()
    load_p.start()
    loads = []
    for l in range(layers):
        pair = (
            pltpu.make_async_copy(memory.at[l], tile.at[l], load_sem.at[2 + 2 * l]),
            pltpu.make_async_copy(grad.at[l], gbuf.at[l], load_sem.at[3 + 2 * l]),
        )
        for c in pair:
            c.start()
        loads.append(pair)

    barrier = pltpu.get_barrier_semaphore()
    peers = [partner] + [z_peer(d) for d in range(1, zs)]
    offsets = [(dx, dy) for dx in (2, 1, 3, 0) for dy in (2, 1, 3, 0) if dx or dy]
    peers += [xy_peer(dx, dy) for dx, dy in offsets]
    for device in peers:
        pl.semaphore_signal(barrier, inc=1, device_id=device, device_id_type=MESH)

    load_q.wait()
    for l in range(layers):
        qg[0, row, l] = shut(q_in[l])
    load_p.wait()
    for l in range(layers):
        p = p_in[l]
        pg[x, y, l] = jnp.concatenate([p[0:8], p[8:16], p[16:24], jnp.zeros((8, 32), F32)], axis=1)
    for l in range(layers):
        for c in loads[l]:
            c.wait()

        @pl.loop(0, rows // 32)
        def _(i):
            at = pl.ds(pl.multiple_of(i * 32, 32), 32)
            t = gbuf[l, at, :].astype(F32) + tile[l, at, :]
            tile[l, at, :] = t
            t1 = t.astype(BF16)
            split[l, at, :] = t1
            split[l, pl.ds(pl.multiple_of(rows + i * 32, 32), 32), :] = (t - t1.astype(F32)).astype(BF16)

    pl.semaphore_wait(barrier, len(peers))

    far_first = sorted(range(1, zs), key=lambda d: -min(d, zs - d))
    near_first = far_first[::-1]

    def shard(phase, l, slot):
        return qg.at[phase, slot] if l is None else qg.at[phase, slot, l]

    def send_shards(phase, l=None):
        mine, i = shard(phase, l, row), l or 0
        for d in far_first:
            start(remote(mine, mine, zq_send.at[phase, i, d], zq_recv.at[phase, i, d], z_peer(d)))
        start(remote(mine, mine, dq_send.at[phase, i, 0], dq_recv.at[phase, i, 0], partner))

    def pass_on(phase, l=None):
        i = l or 0
        for d in near_first:
            there = shard(phase, l, lax.rem(z + zs - d, zs) * 2 + core)
            remote(there, there, zq_send.at[phase, i, d], zq_recv.at[phase, i, d], z_peer(d)).wait_recv()
            start(remote(there, there, dq_send.at[phase, i, d], dq_recv.at[phase, i, d], partner))

    def all_passed(phase, l=None):
        i = l or 0
        for d in range(zs):
            there = shard(phase, l, lax.rem(z + zs - d, zs) * 2 + (1 - core))
            remote(there, there, dq_send.at[phase, i, d], dq_recv.at[phase, i, d], partner).wait_recv()

    send_shards(0)
    for dx, dy in offsets:
        mine = pg.at[x, y]
        start(remote(mine, mine, p_send.at[dx, dy], p_recv.at[dx, dy], xy_peer(dx, dy)))

    def q_columns(phase, l):
        return jnp.concatenate([opened(qg[phase, r, l]) for r in range(2 * zs)], axis=1)

    step = 256
    half = rows // 2
    block = half // 4

    def left_part(l):
        tall[l] = tall_right(q_columns(0, l))
        wide[l] = wide_left(p_rows[l])
        q3 = tall[l, 0:96, :]
        square = dot(q3, q3, NT)
        parts = []
        for h in range(2):
            first, second = (split[l, i * rows + h * half : i * rows + (h + 1) * half, :] for i in range(2))
            acc = dot(first, q3, NT) + dot(second, q3, NT)
            parts.append(acc[:, 0:32] + acc[:, 32:64] + acc[:, 64:96])
        less = dot(wide[l], tall_right(folded(square)))
        return jnp.concatenate(parts, axis=0) - less

    def merge(l):
        for j in range(cols // step):
            at = pl.ds(j * step, step)
            m = tile[l, :, at] - dot(wide[l], tall[l, :, at])
            tile[l, :, at] = m
            m1 = m.astype(BF16)
            split[l, 0:rows, at] = m1
            split[l, rows : 2 * rows, at] = (m - m1.astype(F32)).astype(BF16)

    def halves(v):
        for h in range(2):
            yield jnp.concatenate([v[h * half + b * block : h * half + (b + 1) * block] for b in range(4)], axis=1)

    def exchange(buf, stage, l, h, along_y):
        n, me, peer = (ys, y, y_peer) if along_y else (xs, x, x_peer)
        mine = buf.at[l, h, me]
        for d in sorted(range(1, n), key=lambda d: -min(d, n - d)):
            start(remote(mine, mine, b_send.at[stage, l, h, d], b_recv.at[stage, l, h, d], peer(d)))

    def arrived(buf, stage, l, h, along_y):
        n, me, peer = (ys, y, y_peer) if along_y else (xs, x, x_peer)
        for d in range(1, n):
            there = buf.at[l, h, (me + n - d) % n]
            remote(there, there, b_send.at[stage, l, h, d], b_recv.at[stage, l, h, d], peer(d)).wait_recv()
        total = buf[l, h, 0]
        for i in range(1, n):
            total = total + buf[l, h, i]
        return total

    def first_stage(l):
        part = left_part(l)
        for h, v in enumerate(halves(part)):
            me = y if h == 0 else x
            b1[l, h, me] = v
            exchange(b1, 0, l, h, h == 0)

    def second_stage(l):
        for h in range(2):
            total = arrived(b1, 0, l, h, h == 0)
            me = x if h == 0 else y
            b2[l, h, me] = total
            exchange(b2, 1, l, h, h == 1)

    pass_on(0)
    for dx, dy in offsets[::-1]:
        there = pg.at[lax.rem(x + xs - dx, xs), lax.rem(y + ys - dy, ys)]
        remote(there, there, p_send.at[dx, dy], p_recv.at[dx, dy], xy_peer(dx, dy)).wait_recv()
    for l in range(layers):
        for c in range(xs * ys):
            v = pg[c // ys, c % ys, l]
            p_rows[l, 24 * c : 24 * c + 24, :] = jnp.concatenate([v[:, 32 * b : 32 * b + 32] for b in range(3)], axis=0)
    all_passed(0)
    first_stage(0)
    first_stage(1)
    merge(0)
    merge(1)
    second_stage(0)
    second_stage(1)

    def right_part(l):
        for h in range(2):
            total = arrived(b2, 1, l, h, h == 1)
            for b in range(4):
                left[l, h * half + b * block : h * half + (b + 1) * block, :] = total[:, 32 * b : 32 * b + 32]
        t1, t2, t3 = (t.astype(BF16) for t in pieces(left[l].T))
        lhs = jnp.concatenate([t1, t2, t3], axis=0)
        grams = dot(lhs, lhs, NT)
        g = folded(grams)
        gd[l, core] = jnp.concatenate([g[8 * i : 8 * i + 8] for i in range(4)], axis=1)
        mine = gd.at[l, core]
        start(remote(mine, mine, gd_send.at[l], gd_recv.at[l], partner))
        fulls = []
        for h in range(2):
            at = pl.ds(h * cols // 2, cols // 2)
            fulls.append(dot(lhs, split[l, 0:rows, at]) + dot(lhs, split[l, rows : 2 * rows, at]))
        full = jnp.concatenate(fulls, axis=1)
        r = full[0:32] + full[32:64] + full[64:96]
        for s in range(2 * zs):
            rb[l, s % 2, s // 2] = shut(r[:, 96 * s : 96 * s + 96])
        start(remote(rb.at[l, 1 - core], rd.at[l], rd_send.at[l], rd_recv.at[l], partner))

    def send_gram(l):
        there = gd.at[l, 1 - core]
        remote(there, there, gd_send.at[l], gd_recv.at[l], partner).wait_recv()
        gz[l, z] = gd[l, 0] + gd[l, 1]
        mine = gz.at[l, z]
        for d in far_first:
            start(remote(mine, mine, gz_send.at[l, d], gz_recv.at[l, d], z_peer(d)))

    def scatter(l):
        remote(rb.at[l, 1 - core], rd.at[l], rd_send.at[l], rd_recv.at[l], partner).wait_recv()
        rs[l] = rb[l, core] + rd[l]
        for d in far_first:
            to = (z + d) % zs
            start(remote(rs.at[l, to], rr.at[l, z], rz_send.at[l, d], rz_recv.at[l, d], z_peer(d)))
        rr[l, z] = rs[l, z]

    right_part(0)
    send_gram(0)
    scatter(0)
    right_part(1)
    scatter(1)
    send_gram(1)

    def gather(l):
        for d in near_first:
            there = rr.at[l, (z + zs - d) % zs]
            remote(rs.at[l, 0], there, rz_send.at[l, d], rz_recv.at[l, d], z_peer(d)).wait_recv()
        total = rr[l, 0]
        for i in range(1, zs):
            total = total + rr[l, i]
        qg[1, row, l] = total
        send_shards(1, l)

    gather(0)
    gather(1)

    def whole_gram(l):
        for d in range(1, zs):
            there = gz.at[l, (z + zs - d) % zs]
            remote(there, there, gz_send.at[l, d], gz_recv.at[l, d], z_peer(d)).wait_recv()
        g = gz[l, 0]
        for i in range(1, zs):
            g = g + gz[l, i]
        return jnp.concatenate([g[:, 32 * i : 32 * i + 32] for i in range(4)], axis=0)

    for l in range(layers):
        wide[l] = wide_left(left[l])
    inverses = inverse_factors([whole_gram(l) for l in range(layers)])
    for l in range(layers):
        inverse = inverses[l]
        tall_inverse = tall_right(inverse)
        p = dot(wide[l], wide_right(inverse), NT)
        p_rows[l] = p
        side = wide_out if l else wide.at[0]
        side[...] = wide_left(dot(wide_left(p), tall_inverse))
        share = rows // (xs * ys)
        p_new[l] = p_rows[l, pl.ds(pl.multiple_of(col * share, 8), share), :]
        q_new[l] = dot(wide_left(inverse), tall_right(opened(qg[1, row, l])))
    for copy in sent:
        copy.wait_send()
    sent.clear()
    for l in range(layers):
        pass_on(1, l)
    all_passed(1, 0)
    tall[0] = tall_right(q_columns(1, 0))
    for j in range(cols // step):
        at = pl.ds(j * step, step)
        tile[0, :, at] = tile[0, :, at] - dot(wide[0], tall[0, :, at])
    all_passed(1, 1)
    right_out[...] = q_columns(1, 1)
    for copy in sent:
        copy.wait_send()


def error_kernel(merged, wide, right, p_in, q_in, p_new, q_new, error, buf, tall, out_sem, small_sem):
    rows, cols = buf.shape
    step = rows // 3
    copies = [pltpu.make_async_copy(merged.at[0], error.at[0], small_sem.at[2])]
    copies += [
        pltpu.make_async_copy(p_in, p_new, small_sem.at[0]),
        pltpu.make_async_copy(q_in, q_new, small_sem.at[1]),
    ]
    for c in copies:
        c.start()
    tall[...] = tall_right(right[...])
    for i in range(3):
        at = pl.ds(i * step, step)
        buf[at, :] = merged[1, at, :] - dot(wide[at, :], tall[...])
        copy = pltpu.make_async_copy(buf.at[at, :], error.at[1, at, :], out_sem.at[i])
        copy.start()
        copies.append(copy)
    for c in copies:
        c.wait()


def shards(xs, ys, zs, grad, memory, p_prev, q_prev):
    layers, rows, cols = grad.shape
    rank = p_prev.shape[2]
    wire = 24
    dma = pltpu.SemaphoreType.DMA
    hbm = pl.BlockSpec(memory_space=pltpu.HBM)
    vmem = pl.BlockSpec(memory_space=pltpu.VMEM)
    block = rows // 8

    def body(*refs):
        factor_kernel(zs, xs, ys, *refs)

    merged, wide, right, p_new, q_new = pl.pallas_call(
        body,
        out_shape=(
            jax.ShapeDtypeStruct((layers, rows, cols), F32),
            jax.ShapeDtypeStruct((rows, 6 * rank), BF16),
            jax.ShapeDtypeStruct((rank, cols), F32),
            jax.ShapeDtypeStruct(p_prev.shape, F32),
            jax.ShapeDtypeStruct(q_prev.shape, F32),
        ),
        in_specs=[hbm] * 4,
        out_specs=(vmem,) * 5,
        scratch_shapes=[
            pltpu.VMEM(q_prev.shape, F32),
            pltpu.VMEM(p_prev.shape, F32),
            pltpu.VMEM((layers, rows, cols), BF16),
            pltpu.VMEM((layers, 2 * rows, cols), BF16),
            pltpu.VMEM((2, 2 * zs, layers, wire, 128), F32),
            pltpu.VMEM((xs, ys, layers, 8, 128), F32),
            pltpu.VMEM((layers, rows, rank), F32),
            pltpu.VMEM((layers, rows, 6 * rank), BF16),
            pltpu.VMEM((layers, 6 * rank, cols), BF16),
            pltpu.VMEM((layers, 2, 4, block, 128), F32),
            pltpu.VMEM((layers, 2, 4, block, 128), F32),
            pltpu.VMEM((layers, rows, rank), F32),
            pltpu.VMEM((layers, 2, 8, 128), F32),
            pltpu.VMEM((layers, zs, 8, 128), F32),
            pltpu.VMEM((layers, 2, zs, wire, 128), F32),
            pltpu.VMEM((layers, zs, wire, 128), F32),
            pltpu.VMEM((layers, zs, wire, 128), F32),
            pltpu.VMEM((layers, zs, wire, 128), F32),
            dma((2 + 2 * layers,)),
            dma((2, layers, zs)),
            dma((2, layers, zs)),
            dma((2, layers, zs)),
            dma((2, layers, zs)),
            dma((xs, ys)),
            dma((xs, ys)),
            dma((2, layers, 2, 4)),
            dma((2, layers, 2, 4)),
            dma((layers,)),
            dma((layers,)),
            dma((layers, zs)),
            dma((layers, zs)),
            dma((layers,)),
            dma((layers,)),
            dma((layers, zs)),
            dma((layers, zs)),
        ],
        compiler_params=pltpu.CompilerParams(
            collective_id=0, has_side_effects=True, vmem_limit_bytes=28 * 1024 * 1024
        ),
        name="factors",
    )(*(pltpu.with_memory_space_constraint(v, pltpu.HBM) for v in (grad, memory, p_prev, q_prev)))
    return pl.pallas_call(
        error_kernel,
        out_shape=(
            jax.ShapeDtypeStruct(p_prev.shape, F32),
            jax.ShapeDtypeStruct(q_prev.shape, F32),
            jax.ShapeDtypeStruct((layers, rows, cols), F32),
        ),
        in_specs=[vmem] * 5,
        out_specs=(hbm,) * 3,
        scratch_shapes=[
            pltpu.VMEM((rows, cols), F32),
            pltpu.VMEM((6 * rank, cols), BF16),
            dma((3,)),
            dma((3,)),
        ],
        compiler_params=pltpu.CompilerParams(vmem_limit_bytes=32 * 1024 * 1024),
        name="error",
    )(merged, wide, right, p_new, q_new)


def solution(mesh):
    placed = (
        P(None, "row", "col"),
        P(None, "row", "col"),
        P(None, ("row", "col"), None),
        P(None, ("col", "row"), None),
    )
    xs = ys = 4
    zs = mesh.shape["row"] // 2

    def body(grad, memory, p_prev, q_prev):
        p_new, q_new, error = shards(xs, ys, zs, grad, memory, p_prev, jnp.swapaxes(q_prev, 1, 2))
        return p_new, jnp.swapaxes(q_new, 1, 2), error

    return jax.shard_map(
        body,
        mesh=mesh,
        in_specs=placed,
        out_specs=(
            P(None, ("row", "col"), None),
            P(None, ("col", "row"), None),
            P(None, "row", "col"),
        ),
        check_vma=False,
    )
```
